256 devices in a mesh: col: 128 (over x, z, y), sec: 2 (over core).
Axes of the slice: x: 4, y: 4, z: 8, core: 2. Of those that a mesh axis runs over, the one named last changes fastest.
Arguments:
- mps: bfloat16 [128, 96, 6, 6, 96], P('col', 'sec'), may hold values from -6 to 6
- ket: bfloat16 [128, 6, 6, 6, 6, 2], P('col'), may hold values from -6 to 6
- left_proj: bfloat16 [128, 96, 96, 6, 6], P('col', 'sec'), may hold values from -0.109375 to 0.109375
- right_proj: bfloat16 [128, 96, 6, 6, 96], P('col', None, None, None, 'sec'), may hold values from -0.109375 to 0.109375
- bond_charge: int32 [128, 96], P('col'), may hold values from 0 to 5
- new_charge: int32 [128, 96], P('col'), may hold values from 0 to 5
- link_charge: int32 [128, 6], P('col'), may hold values from 0 to 2
- vert_charge: int32 [128, 2, 6], P('col'), may hold values from 0 to 2
Outputs:
- new_mps: bfloat16 [128, 96, 6, 6, 96], P('col', 'sec')
- log_norm: float32 [], replicated
The draws below stay inside these ranges and needn't reach their ends.
All inputs are finite; a program needn't handle non-finite values.
Results may differ from the reference program's by a relative error of at most 0.0064.
Values may be sent and summed in bfloat16 or wider, within the bound.
A program may use at most 192 MiB of HBM per device.

```python
import jax
import jax.numpy as jnp
from jax import lax

CHI = 96
D = 6
P_SIZE = 2
SITES = 128


def with_ends(values, key, least, top_value):
    dims = values.shape
    index_at = [jax.random.randint(jax.random.fold_in(key, axis), (), 0, dims[axis]) for axis in range(len(dims))]
    values = values.at[tuple(index_at)].set(least)
    longest = dims.index(max(dims))
    index_at[longest] = (index_at[longest] + 1) % dims[longest]
    return values.at[tuple(index_at)].set(top_value)


def steps_of(rng, extent, split, low, largest):
    loudness = 1.0
    for dim, blocks in split:
        draws = jax.random.uniform(jax.random.fold_in(jax.random.fold_in(rng, 6), dim), (blocks,), jnp.float32, low / len(split), largest / len(split))
        loudness = loudness * jnp.repeat(jnp.exp(draws), extent[dim] // blocks).reshape((-1,) + (1,) * (len(extent) - 1 - dim))
    return loudness


def normal_values(stream_key, extent, deviation, most, cuts=(), held_as=jnp.bfloat16):
    entries = jax.random.normal(stream_key, extent, jnp.float32) * deviation
    if len(cuts) > 0:
        entries = steps_of(stream_key, extent, cuts, -0.22, 0.18) * entries
    return jnp.clip(entries, min=-most, max=most).astype(held_as)


def setup_inputs(seed: int = 0) -> dict:
    key_of = jax.random.split(jax.random.key(seed), 9)
    return {
        "mps": normal_values(key_of[0], (SITES, CHI, D, D, CHI), 1.0, 6.0, ((0, 128), (1, 2))),
        "ket": normal_values(key_of[1], (SITES, D, D, D, D, P_SIZE), 1.0, 6.0, ((0, 128),)),
        "left_proj": normal_values(key_of[2], (SITES, CHI, CHI, D, D), (CHI * D * D) ** -0.5, 0.109375, ((0, 128), (1, 2))),
        "right_proj": normal_values(key_of[3], (SITES, CHI, D, D, CHI), (CHI * D * D) ** -0.5, 0.109375, ((0, 128), (4, 2))),
        "bond_charge": with_ends(jax.random.randint(key_of[4], (SITES, CHI), 0, 6), jax.random.fold_in(key_of[4], 1), 0, 5).astype(jnp.int32),
        "new_charge": with_ends(jax.random.randint(key_of[5], (SITES, CHI), 0, 6), jax.random.fold_in(key_of[5], 1), 0, 5).astype(jnp.int32),
        "link_charge": with_ends(jax.random.randint(key_of[6], (SITES, D), 0, 3), jax.random.fold_in(key_of[6], 1), 0, 2).astype(jnp.int32),
        "vert_charge": with_ends(jax.random.randint(key_of[7], (SITES, 2, D), 0, 3), jax.random.fold_in(key_of[7], 1), 0, 2).astype(jnp.int32),
    }


def absorb(mps_site, ket_site, left_site, right_site, charge_here, charge_next, fresh_here, fresh_next, link_here, link_next, vertical):
    upper = vertical[0]
    lower = vertical[1]
    physical = jnp.arange(ket_site.shape[4], dtype=jnp.int32)
    keep_mps = charge_here[:, None, None, None] + upper[None, :, None, None] - upper[None, None, :, None] == charge_next[None, None, None, :]
    masked_mps = jnp.where(keep_mps, mps_site, jnp.zeros_like(mps_site))
    keep_ket = upper[:, None, None, None, None] + link_here[None, :, None, None, None] == lower[None, None, :, None, None] + link_next[None, None, None, :, None] + physical[None, None, None, None, :]
    masked_ket = jnp.where(keep_ket, ket_site, jnp.zeros_like(ket_site))
    keep_left = fresh_here[:, None, None, None] == charge_here[None, :, None, None] + link_here[None, None, :, None] - link_here[None, None, None, :]
    masked_left = jnp.where(keep_left, left_site, jnp.zeros_like(left_site))
    keep_right = charge_next[:, None, None, None] + link_next[None, :, None, None] - link_next[None, None, :, None] == fresh_next[None, None, None, :]
    masked_right = jnp.where(keep_right, right_site, jnp.zeros_like(right_site))
    ket_wide = masked_ket.astype(jnp.float32)
    first = jnp.einsum('xalm,auvb->xlmuvb', masked_left.astype(jnp.float32), masked_mps.astype(jnp.float32)).astype(jnp.bfloat16)
    second = jnp.einsum('xlmuvb,uldrp->xmvbdrp', first.astype(jnp.float32), ket_wide).astype(jnp.bfloat16)
    third = jnp.einsum('xmvbdrp,vmesp->xbdres', second.astype(jnp.float32), ket_wide).astype(jnp.bfloat16)
    return jnp.einsum('xbdres,brsy->xdey', third.astype(jnp.float32), masked_right.astype(jnp.float32))

def reference(mps, ket, left_proj, right_proj, bond_charge, new_charge, link_charge, vert_charge):

    def following(array):
        return jnp.roll(array, -1, axis=0)
    items = (mps, ket, left_proj, following(right_proj), bond_charge, following(bond_charge), new_charge, following(new_charge), link_charge, following(link_charge), vert_charge)

    def single(item):
        return absorb(*item)
    image = lax.map(single, items)
    count = CHI * D * D * CHI
    meansq = lax.optimization_barrier(jnp.sum(image * image, axis=(1, 2, 3, 4))) / count
    scale = lax.rsqrt(meansq + 1e-06)
    new_mps = (image * scale[:, None, None, None, None]).astype(jnp.bfloat16)
    log_norm = jnp.mean(0.5 * jnp.log(meansq + 1e-06))
    return (new_mps, log_norm)
```

```python
import numpy as np

import jax
import jax.numpy as jnp
from jax import lax
from jax.experimental import pallas as pl
from jax.experimental.pallas import tpu as pltpu
from jax.sharding import Mesh
from jax.sharding import PartitionSpec as P

COL = ("col_0", "col_1", "col_2")
F32, BF16, I32 = jnp.float32, jnp.bfloat16, jnp.int32
MESH = pl.DeviceIdType.MESH
FORWARD_AT = 9


def operator_tables():
    e2 = np.zeros((432, 128), np.float32)
    f2 = np.zeros((48, 256), np.float32)
    k2 = np.zeros((432, 256), np.float32)
    rows_m = np.full(432, -1)
    cols_m = np.full(256, -2)
    for d in range(6):
        for r in range(6):
            for m in range(6):
                for p in range(2):
                    row = ((d * 6 + r) * 6 + m) * 2 + p
                    e2[row, (d * 6 + r) * 2 + p] = 1
                    rows_m[row] = m
    for u in range(6):
        for l in range(6):
            for m in range(6):
                f2[u * 6 + l, u * 40 + l * 6 + m] = 1
                cols_m[u * 40 + l * 6 + m] = m
    k2[:] = rows_m[:, None] == cols_m[None, :]
    e3 = np.zeros((2, 96, 128), np.float32)
    f3 = np.zeros((2, 48, 144), np.float32)
    rows_r = np.full(96, -1)
    cols_r = np.full(144, -2)
    for r in range(2):
        for s in range(6):
            for e in range(6):
                row = (r * 6 + s) * 8 + e
                rows_r[row] = r
                for p in range(2):
                    e3[p, row, (e * 6 + s) * 2 + p] = 1
        for v in range(6):
            for m in range(6):
                for p in range(2):
                    col = v * 24 + r * 12 + m * 2 + p
                    cols_r[col] = r
                    f3[p, v * 6 + m, col] = 1
    k3 = (rows_r[:, None] == cols_r[None, :]).astype(np.float32)
    gu = np.zeros((48, 128), np.float32)
    gl = np.zeros((48, 128), np.float32)
    for u in range(6):
        for l in range(6):
            gu[u * 6 + l, u] = 1
            gl[u * 6 + l, l] = 1
    hd = np.zeros((128, 128), np.float32)
    hr = np.zeros((128, 128), np.float32)
    hp = np.zeros((8, 128), np.float32)
    for d in range(6):
        for r in range(6):
            for p in range(2):
                hd[d, (d * 6 + r) * 2 + p] = 1
                hr[r, (d * 6 + r) * 2 + p] = 1
                hp[:, (d * 6 + r) * 2 + p] = p
    narrow = lambda t: jnp.asarray(t, BF16)
    return [narrow(e2), narrow(f2), jnp.asarray(k2), narrow(e3), narrow(f3), jnp.asarray(k3),
            jnp.asarray(gu), jnp.asarray(gl), narrow(hd), narrow(hr), jnp.asarray(hp)]


def column(row):
    return jnp.transpose(jnp.broadcast_to(row, (128, 128)))


def kernel(sizes, link_s, vert_s, bond, fresh, link, vert, ketm, e2, f2, k2, e3, f3, k3, gu, gl, hd, hr, hp,
           mps_h, left_h, right_h, out_h, log_out,
           rows, bond_n, fresh_n, link_n, left_v, MB, RB, LF, L2F, L2, MS, RS, KM, KB2, KB3, W1, W2, W3, IMG, OUT,
           SQ, SA, SB,
           lsem, csend, crecv, msend, mrecv, rsend, rrecv, fsend, frecv, qsend, qrecv, asend, arecv, bsend, brecv,
           osem):
    nx, nz, ny, _ = sizes
    x, z, y = lax.axis_index("col_0"), lax.axis_index("col_1"), lax.axis_index("col_2")
    sec = lax.axis_index("sec")
    other = 1 - sec
    count = nx * nz * ny
    site = (x * nz + z) * ny + y

    def place(j):
        return {"col_0": lax.div(j, nz * ny), "col_1": lax.rem(lax.div(j, ny), nz), "col_2": lax.rem(j, ny)}

    before = place(lax.rem(site + count - 1, count))
    after = place(lax.rem(site + 1, count))
    partner = {"sec": other}
    plane = x * ny + y
    plane_n = nx * ny

    def plane_peer(k):
        q = lax.rem(plane + k, plane_n)
        return {"col_0": lax.div(q, ny), "col_2": lax.rem(q, ny)}

    def line_peer(k):
        return {"col_1": lax.rem(z + k, nz)}

    left_copy = pltpu.make_async_copy(left_h, left_v, lsem.at[0])
    left_copy.start()
    mps_copy = pltpu.make_async_copy(mps_h, MB.at[sec], lsem.at[1])
    mps_copy.start()

    barrier = pltpu.get_barrier_semaphore()
    peers = [partner, before, after]
    peers += [plane_peer(k) for k in range(1, plane_n)]
    peers += [line_peer(k) for k in range(1, nz)]
    for peer in peers:
        pl.semaphore_signal(barrier, inc=1, device_id=peer, device_id_type=MESH)
    pl.semaphore_wait(barrier, len(peers))

    def remote(src, dst, send, recv, peer):
        return pltpu.make_async_remote_copy(src_ref=src, dst_ref=dst, send_sem=send, recv_sem=recv,
                                            device_id=peer, device_id_type=MESH)

    charges = [remote(bond, bond_n, csend.at[0], crecv.at[0], before),
               remote(fresh, fresh_n, csend.at[1], crecv.at[1], before),
               remote(link, link_n, csend.at[2], crecv.at[2], before)]
    for c in charges:
        c.start()
    mps_send = remote(mps_h, MB.at[sec], msend, mrecv, partner)
    mps_send.start()
    right_send = remote(right_h, RB.at[sec], rsend, rrecv, before)
    right_send.start()
    right_forward = remote(RB.at[sec], RB.at[sec], fsend, frecv, partner)

    rows[...] = jnp.zeros_like(rows)
    rows[0:1, 0:96] = bond[...]
    rows[1:2, 0:96] = fresh[...]
    qb = rows[0:1, :]
    col_qb = column(qb)
    col_fresh = column(rows[1:2, :])
    LF[...] = jnp.zeros_like(LF)
    L2F[...] = jnp.zeros_like(L2F)
    fresh_half = jnp.where(sec == 0, col_fresh[0:48, :], col_fresh[48:96, :])
    left_diff = fresh_half[:, :96] - qb[:, :96]
    left_copy.wait()
    for l in range(6):
        for m in range(6):
            keep = left_diff == link_s[0, l] - link_s[0, m]
            LF[pl.ds((l * 6 + m) * 48, 48), 0:96] = jnp.where(keep, left_v[l, m].astype(F32), 0.0)
    for i in range(48):
        L2F[pl.ds(40 * i, 36), :] = LF[pl.ds(i, 36, stride=48), :]
    L2[...] = L2F[...].astype(BF16)
    W1[:, :, 240:256, :] = jnp.zeros((24, 6, 16, 256), BF16)
    MS[...] = jnp.zeros_like(MS)
    RS[...] = jnp.zeros_like(RS)
    KM[...] = jnp.zeros_like(KM)

    for c in charges:
        c.wait_recv()
    rows[2:3, 0:96] = bond_n[...]
    rows[3:4, 0:96] = fresh_n[...]
    rows[4:5, 0:6] = link[...]
    rows[5:6, 0:6] = link_n[...]
    rows[6:8, 0:6] = vert[0]
    qbn = rows[2:3, :]

    charge_rows = rows[...].astype(F32)
    ket_rows = jnp.sum(gu[...] * charge_rows[6:7, :] + gl[...] * charge_rows[4:5, :], axis=1, keepdims=True)
    lower = jnp.broadcast_to(charge_rows[7:8, :], (8, 128)).astype(BF16)
    ahead = jnp.broadcast_to(charge_rows[5:6, :], (8, 128)).astype(BF16)
    ket_cols = (jnp.dot(lower, hd[...], preferred_element_type=F32)
                + jnp.dot(ahead, hr[...], preferred_element_type=F32) + hp[...])[0:1, :]
    keep_ket = jnp.abs(ket_rows - ket_cols) < 0.5
    KM[0:36, 0:72] = jnp.where(keep_ket[0:36, 0:72], ketm[...].astype(F32), 0.0).astype(BF16)
    spread = lax.dot_general(e2[...], KM[...], (((1,), (1,)), ((), ())), preferred_element_type=F32)
    KB2[...] = (jnp.dot(spread.astype(BF16), f2[...], preferred_element_type=F32) * k2[...]).astype(BF16)
    total = None
    for p in range(2):
        spread = lax.dot_general(e3[p], KM[...], (((1,), (1,)), ((), ())), preferred_element_type=F32)
        part = jnp.dot(spread.astype(BF16), f3[p], preferred_element_type=F32)
        total = part if total is None else total + part
    KB3[...] = (total * k3[...]).astype(BF16)

    bond_diff = qbn[:, :96] - col_qb[:96, :96]
    mps_copy.wait()
    mps_send.wait_recv()
    for u in range(6):
        for v in range(6):
            keep = bond_diff == vert_s[0, 0, u] - vert_s[0, 0, v]
            t = jnp.concatenate([MB[0, u, v], MB[1, u, v]], axis=0).astype(F32)
            MS[(u // 2) * 6 + v, 0:96, pl.ds((u % 2) * 128, 96)] = jnp.where(keep, t, 0.0).astype(BF16)

    def step1(i, carry):
        up, v = lax.div(i, 6), lax.rem(i, 6)
        rhs = MS[i]
        for c in range(12):
            o = jnp.dot(L2[c * 160:(c + 1) * 160, :], rhs, preferred_element_type=F32)
            for k in range(4):
                s = 4 * c + k
                t = jnp.concatenate([o[40 * k:40 * k + 40, :128], o[40 * k:40 * k + 40, 128:]], axis=0)
                W1[s // 2, v, pl.ds(pl.multiple_of(up * 80, 16), 80),
                   (s % 2) * 128:(s % 2) * 128 + 128] = t.astype(BF16)
        return carry

    lax.fori_loop(0, 18, step1, 0)

    def do2(xp, slot):
        for vp in range(3):
            oa = jnp.dot(KB2[...], W1[xp, 2 * vp], preferred_element_type=F32)
            ob = jnp.dot(KB2[...], W1[xp, 2 * vp + 1], preferred_element_type=F32)
            for g in range(18):
                t = jnp.concatenate([oa[24 * g:24 * g + 24], ob[24 * g:24 * g + 24]], axis=0)
                W2[slot, g, 48 * vp:48 * vp + 48, :] = t.astype(BF16)

    def do3(xp, slot):
        for g in range(18):
            d, rp = g // 3, g % 3
            o = jnp.dot(KB3[...], W2[slot, g], preferred_element_type=F32)
            for i in range(12):
                rs = (2 * rp + i // 6) * 6 + i % 6
                t = jnp.concatenate([o[8 * i:8 * i + 8, :128], o[8 * i:8 * i + 8, 128:]], axis=0)
                W3[pl.ds(pl.multiple_of(xp * 96 + d * 16, 16), 16), rs * 128:rs * 128 + 128] = t.astype(BF16)

    do2(0, 0)

    def step23(xp, carry):
        slot = lax.rem(xp, 2)

        @pl.when(xp == FORWARD_AT)
        def _():
            right_send.wait_recv()
            right_forward.start()

        do2(xp, slot)
        do3(xp - 1, 1 - slot)
        return carry

    lax.fori_loop(1, 24, step23, 0)
    do3(23, 1)

    right_forward.wait_recv()
    col_qy = column(rows[3:4, :])
    right_diff = col_qy[:96, :96] - qbn[:, :96]
    ahead_row = rows[5:6, :]
    for r in range(6):
        for s in range(6):
            keep = right_diff == ahead_row[:, r:r + 1] - ahead_row[:, s:s + 1]
            t = jnp.concatenate([RB[0, r, s], RB[1, r, s]], axis=0).astype(F32)
            rs = r * 6 + s
            RS[:, rs * 128:rs * 128 + 96] = jnp.where(keep, t, 0.0).astype(BF16)

    def step4(c, acc):
        o = lax.dot_general(W3[pl.ds(pl.multiple_of(c * 384, 128), 384), :], RS[...],
                            (((1,), (1,)), ((), ())), preferred_element_type=F32)
        for k in range(4):
            for d in range(6):
                for h in range(2):
                    row = (c * 8 + 2 * k + h) * 48 + d * 8
                    at = k * 96 + d * 16 + h * 8
                    tile = o[at:at + 8]
                    IMG[pl.ds(pl.multiple_of(row, 8), 8), 0:96] = tile
                    acc = acc + tile * tile
        return acc

    acc = lax.fori_loop(0, 6, step4, jnp.zeros((8, 96), F32))
    mine = jnp.sum(jnp.sum(acc, axis=0, keepdims=True), axis=1, keepdims=True)
    SQ[sec] = jnp.broadcast_to(mine, (1, 128))
    square_send = remote(SQ.at[sec], SQ.at[sec], qsend, qrecv, partner)
    square_send.start()
    square_send.wait_recv()
    meansq = (SQ[0] + SQ[1]) / 331776.0
    scale = lax.rsqrt(meansq + 1e-06)
    SA[plane] = 0.5 * jnp.log(meansq + 1e-06)

    plane_sends = [remote(SA.at[plane], SA.at[plane], asend.at[k], arecv.at[k], plane_peer(k))
                   for k in range(1, plane_n)]
    for c in plane_sends:
        c.start()

    for d in range(6):
        for e in range(6):
            t = IMG[pl.ds(d * 8 + e, 48, stride=48), 0:96]
            OUT[d, e] = (t * scale[:, 0:96]).astype(BF16)
    out_copy = pltpu.make_async_copy(OUT, out_h, osem)
    out_copy.start()

    for c in plane_sends:
        c.wait_recv()
    total = SA[0]
    for k in range(1, plane_n):
        total = total + SA[k]
    SB[z] = total
    line_sends = [remote(SB.at[z], SB.at[z], bsend.at[k], brecv.at[k], line_peer(k)) for k in range(1, nz)]
    for c in line_sends:
        c.start()
    for c in line_sends:
        c.wait_recv()
    total = SB[0]
    for k in range(1, nz):
        total = total + SB[k]
    log_out[...] = total / float(count)

    for c in charges + [mps_send, right_send, right_forward, square_send] + plane_sends + line_sends:
        c.wait_send()
    out_copy.wait()


def local(sizes, mps, ket, left_proj, right_proj, bond_charge, new_charge, link_charge, vert_charge):
    nx, nz, ny, _ = sizes
    mps_v = mps[0].transpose(1, 2, 0, 3)
    left_v = left_proj[0].transpose(2, 3, 0, 1)
    right_v = right_proj[0].transpose(1, 2, 3, 0)
    ketm = ket.reshape(36, 72)
    tables = operator_tables()
    vm = pl.BlockSpec(memory_space=pltpu.VMEM)
    sm = pl.BlockSpec(memory_space=pltpu.SMEM)
    hbm = pl.BlockSpec(memory_space=pl.ANY)
    dma = pltpu.SemaphoreType.DMA
    out, log_row = pl.pallas_call(
        lambda *refs: kernel(sizes, *refs),
        out_shape=(jax.ShapeDtypeStruct((6, 6, 48, 96), BF16), jax.ShapeDtypeStruct((1, 128), F32)),
        in_specs=[sm, sm] + [vm] * (5 + len(tables)) + [hbm] * 3,
        out_specs=(hbm, vm),
        scratch_shapes=[
            pltpu.VMEM((8, 128), I32),
            pltpu.VMEM((1, 96), I32), pltpu.VMEM((1, 96), I32), pltpu.VMEM((1, 6), I32),
            pltpu.VMEM((6, 6, 48, 96), BF16),
            pltpu.VMEM((2, 6, 6, 48, 96), BF16), pltpu.VMEM((2, 6, 6, 48, 96), BF16),
            pltpu.VMEM((1728, 128), F32), pltpu.VMEM((1920, 128), F32), pltpu.VMEM((1920, 128), BF16),
            pltpu.VMEM((18, 128, 256), BF16), pltpu.VMEM((96, 4608), BF16),
            pltpu.VMEM((48, 128), BF16), pltpu.VMEM((432, 256), BF16), pltpu.VMEM((96, 144), BF16),
            pltpu.VMEM((24, 6, 256, 256), BF16), pltpu.VMEM((2, 18, 144, 256), BF16),
            pltpu.VMEM((2304, 4608), BF16), pltpu.VMEM((2304, 128), F32),
            pltpu.VMEM((6, 6, 48, 96), BF16),
            pltpu.VMEM((2, 1, 128), F32), pltpu.VMEM((nx * ny, 1, 128), F32), pltpu.VMEM((nz, 1, 128), F32),
            dma((2,)), dma((3,)), dma((3,)), dma(()), dma(()), dma(()), dma(()), dma(()), dma(()), dma(()), dma(()),
            dma((nx * ny,)), dma((nx * ny,)), dma((nz,)), dma((nz,)), dma(())],
        compiler_params=pltpu.CompilerParams(
            vmem_limit_bytes=67_043_328, collective_id=0, has_side_effects=True),
    )(link_charge, vert_charge, bond_charge, new_charge, link_charge, vert_charge, ketm, *tables,
      mps_v, left_v, right_v)
    return out.transpose(2, 0, 1, 3)[None], log_row[0, 0]


def solution(mesh):
    if mesh.shape["col"] == 128:
        sizes = (4, 8, 4, mesh.shape["sec"])
    else:
        sizes = (2, mesh.shape["col"] // 4, 2, mesh.shape["sec"])
    torus = Mesh(mesh.devices.reshape(sizes), (*COL, "sec"))
    in_specs = (
        P(COL, "sec", None, None, None),
        P(COL, None, None, None, None, None),
        P(COL, "sec", None, None, None),
        P(COL, None, None, None, "sec"),
        P(COL, None),
        P(COL, None),
        P(COL, None),
        P(COL, None, None),
    )
    out_specs = (P(COL, "sec", None, None, None), P())
    return jax.shard_map(lambda *a: local(sizes, *a), mesh=torus, in_specs=in_specs, out_specs=out_specs,
                         check_vma=False)
```

```python
import numpy as np

import jax
import jax.numpy as jnp
from jax import lax
from jax.experimental import pallas as pl
from jax.experimental.pallas import tpu as pltpu
from jax.sharding import Mesh
from jax.sharding import PartitionSpec as P

COL = ("col_0", "col_1", "col_2")
F32, BF16, I32 = jnp.float32, jnp.bfloat16, jnp.int32
MESH = pl.DeviceIdType.MESH
FORWARD_AT = 3
CHUNK1 = 480
VMEM_LIMIT = 67_043_328


def operator_tables():
    e2 = np.zeros((432, 128), np.float32)
    f2 = np.zeros((48, 256), np.float32)
    rows_m = np.full(432, -1)
    cols_m = np.full(256, -2)
    hd = np.zeros((128, 128), np.float32)
    hr = np.zeros((128, 128), np.float32)
    hp = np.zeros((16, 128), np.float32)
    for d in range(6):
        for r in range(6):
            for p in range(2):
                lane = (2 * d + p) * 8 + r
                hd[d, lane] = 1
                hr[r, lane] = 1
                hp[:, lane] = p
                for m in range(6):
                    row = ((d * 6 + r) * 6 + m) * 2 + p
                    e2[row, lane] = 1
                    rows_m[row] = m
    gu = np.zeros((48, 128), np.float32)
    gl = np.zeros((48, 128), np.float32)
    for u in range(6):
        for l in range(6):
            gu[u * 6 + l, u] = 1
            gl[u * 6 + l, l] = 1
            for m in range(6):
                f2[u * 6 + l, u * 40 + l * 6 + m] = 1
                cols_m[u * 40 + l * 6 + m] = m
    k2 = rows_m[:, None] == cols_m[None, :]
    e3 = np.zeros((2, 96, 128), np.float32)
    f3 = np.zeros((2, 48, 256), np.float32)
    rows_r = np.full(96, -1)
    cols_r = np.full(256, -2)
    for r in range(2):
        for s in range(6):
            for e in range(6):
                row = (r * 6 + s) * 8 + e
                rows_r[row] = r
                for p in range(2):
                    e3[p, row, (2 * e + p) * 8 + s] = 1
        for v in range(6):
            for m in range(6):
                for p in range(2):
                    col = v * 24 + r * 12 + m * 2 + p
                    cols_r[col] = r
                    f3[p, v * 6 + m, col] = 1
    k3 = rows_r[:, None] == cols_r[None, :]
    narrow = np.concatenate([e2, e3.reshape(192, 128), hd, hr, gu, gl, hp])
    wide = np.concatenate([f2, k2, f3.reshape(96, 256), k3])
    return jnp.asarray(narrow, BF16), jnp.asarray(wide, BF16)


def column(row):
    return jnp.transpose(jnp.broadcast_to(row, (128, 128)))


def lane_parts(t):
    lane = lax.broadcasted_iota(I32, (96, 128), 1)
    t = jnp.concatenate([t, jnp.zeros((96, 32), F32)], axis=1)
    r32, r64, r96 = (pltpu.roll(t, n, axis=1) for n in (32, 64, 96))
    first = [t, jnp.where(lane < 64, r96, 0.0), jnp.where(lane < 32, r64, 0.0)]
    second = [jnp.where(lane >= 96, r96, 0.0), jnp.where(lane >= 64, r64, 0.0), jnp.where(lane >= 32, r32, 0.0)]
    return first, second


def kernel(sizes, bond, fresh, link, vert, narrow_h, wide_h, ket_h, mps_h, left_h, right_h, out_h, log_out,
           rows, bond_v, fresh_v, link_v, vert_v, bond_n, fresh_n, link_n, link_s, vert_s,
           narrow, wide, KH, KF, left_v, MB, RB, LF, L2F, L2, MS, RS, KM, KB2, KB3, W1, W2, W3, O4, IMG, OUT,
           SA, SB,
           lsem, csend, crecv, msend, mrecv, rsend, rrecv, fsend, frecv, asend, arecv, bsend, brecv, osem):
    nx, nz, ny, _ = sizes
    x, z, y = lax.axis_index("col_0"), lax.axis_index("col_1"), lax.axis_index("col_2")
    sec = lax.axis_index("sec")
    other = 1 - sec
    count = nx * nz * ny
    site = (x * nz + z) * ny + y

    def place(j):
        return {"col_0": lax.div(j, nz * ny), "col_1": lax.rem(lax.div(j, ny), nz), "col_2": lax.rem(j, ny)}

    before = place(lax.rem(site + count - 1, count))
    after = place(lax.rem(site + 1, count))
    partner = {"sec": other}
    plane = x * ny + y
    plane_n = nx * ny

    def plane_peer(k, flip):
        q = lax.rem(plane + k, plane_n)
        return {"col_0": lax.div(q, ny), "col_2": lax.rem(q, ny), "sec": other if flip else sec}

    def line_peer(k):
        return {"col_1": lax.rem(z + k, nz)}

    barrier = pltpu.get_barrier_semaphore()
    peers = [before, after]
    peers += [plane_peer(k, f) for k in range(plane_n) for f in range(2) if k + f > 0]
    peers += [line_peer(k) for k in range(1, nz)]
    for peer in peers:
        pl.semaphore_signal(barrier, inc=1, device_id=peer, device_id_type=MESH)

    fetched = [pltpu.make_async_copy(src, dst, lsem.at[i]) for i, (src, dst) in enumerate([
        (link, link_s), (bond, bond_v), (fresh, fresh_v), (left_h, left_v), (vert, vert_s), (link, link_v),
        (vert, vert_v), (ket_h, KH), (narrow_h, narrow), (wide_h, wide), (mps_h, MB.at[sec])])]
    for c in fetched:
        c.start()

    rows[...] = jnp.zeros_like(rows)
    LF[...] = jnp.zeros_like(LF)
    L2F[...] = jnp.zeros_like(L2F)
    MS[:, :, 96:128, :] = jnp.zeros((3, 3, 32, 512), BF16)
    MS[:, :, 224:256, :] = jnp.zeros((3, 3, 32, 512), BF16)
    KF[...] = jnp.zeros_like(KF)
    KM[...] = jnp.zeros_like(KM)

    for c in fetched[:4]:
        c.wait()
    rows[0:1, 0:96] = bond_v[...]
    rows[1:2, 0:96] = fresh_v[...]
    qb = rows[0:1, :]
    col_qb = column(qb)
    col_fresh = column(rows[1:2, :])
    fresh_half = jnp.where(sec == 0, col_fresh[0:48, :], col_fresh[48:96, :])
    left_diff = fresh_half[:, :96] - qb[:, :96]
    for l in range(6):
        for m in range(6):
            keep = left_diff == link_s[0, l] - link_s[0, m]
            LF[pl.ds((l * 6 + m) * 48, 48), 0:96] = jnp.where(keep, left_v[l, m].astype(F32), 0.0)

    pl.semaphore_wait(barrier, len(peers))

    def remote(src, dst, send, recv, peer):
        return pltpu.make_async_remote_copy(src_ref=src, dst_ref=dst, send_sem=send, recv_sem=recv,
                                            device_id=peer, device_id_type=MESH)

    charges = [remote(bond, bond_n, csend.at[0], crecv.at[0], before),
               remote(link, link_n, csend.at[1], crecv.at[1], before),
               remote(fresh, fresh_n, csend.at[2], crecv.at[2], before)]
    for c in charges:
        c.start()
    mps_send = remote(mps_h, MB.at[sec], msend, mrecv, partner)
    mps_send.start()
    right_send = remote(right_h, RB.at[sec], rsend, rrecv, before)
    right_send.start()
    right_forward = remote(RB.at[sec], RB.at[sec], fsend, frecv, partner)

    for i in range(48):
        L2F[i % 4, pl.ds(40 * (i // 4), 36), :] = LF[pl.ds(i, 36, stride=48), :]
    L2[...] = L2F[...].astype(BF16)
    W1[:, :, 240:256, :] = jnp.zeros((6, 6, 16, 768), BF16)
    for c in fetched[4:]:
        c.wait()
    KF[:, 0:6] = KH[...].astype(F32)
    ket = None
    for i in range(12):
        part = KF[pl.ds(i, 36, stride=12), :]
        part = part if i == 0 else pltpu.roll(part, 8 * i, axis=1)
        ket = part if ket is None else ket + part

    for c in charges:
        c.wait_recv()
    rows[2:3, 0:96] = bond_n[...]
    rows[3:4, 0:96] = fresh_n[...]
    rows[4:5, 0:6] = link_v[...]
    rows[5:6, 0:6] = link_n[...]
    rows[6:8, 0:6] = vert_v[0]
    qbn = rows[2:3, :]

    def operators():
        charge_rows = rows[...].astype(F32)
        ket_rows = jnp.sum(narrow[880:928, :].astype(F32) * charge_rows[6:7, :]
                           + narrow[928:976, :].astype(F32) * charge_rows[4:5, :], axis=1, keepdims=True)
        lower = jnp.broadcast_to(charge_rows[7:8, :], (16, 128)).astype(BF16)
        ahead = jnp.broadcast_to(charge_rows[5:6, :], (16, 128)).astype(BF16)
        ket_cols = (jnp.dot(lower, narrow[624:752, :], preferred_element_type=F32)
                    + jnp.dot(ahead, narrow[752:880, :], preferred_element_type=F32)
                    + narrow[976:992, :].astype(F32))[0:1, :]
        keep = jnp.abs(ket_rows[0:36] - ket_cols) < 0.5
        KM[0:36, :] = jnp.where(keep, ket, 0.0).astype(BF16)
        spread = lax.dot_general(narrow[0:432, :], KM[...], (((1,), (1,)), ((), ())), preferred_element_type=F32)
        KB2[...] = (jnp.dot(spread.astype(BF16), wide[0:48, :], preferred_element_type=F32)
                    * wide[48:480, :].astype(F32)).astype(BF16)
        total = None
        for p in range(2):
            spread = lax.dot_general(narrow[432 + 96 * p:528 + 96 * p, :], KM[...], (((1,), (1,)), ((), ())),
                                     preferred_element_type=F32)
            part = jnp.dot(spread.astype(BF16), wide[480 + 48 * p:528 + 48 * p, :], preferred_element_type=F32)
            total = part if total is None else total + part
        KB3[...] = (total * wide[576:672, :].astype(F32)).astype(BF16)

    operators()
    bond_diff = qbn[:, :96] - col_qb[:96, :96]
    mps_send.wait_recv()

    def boundary(i):
        up, vp = i // 3, i % 3
        for v in (2 * vp, 2 * vp + 1):
            for u in (2 * up, 2 * up + 1):
                keep = bond_diff == vert_s[0, 0, u] - vert_s[0, 0, v]
                t = jnp.concatenate([MB[0, u, v], MB[1, u, v]], axis=0).astype(F32)
                first, second = lane_parts(jnp.where(keep, t, 0.0))
                at = ((u % 2) + 2 * (v % 2)) * 128
                for k in range(3):
                    MS[i % 3, k, 0:96, at:at + 128] = first[k].astype(BF16)
                    MS[i % 3, k, 128:224, at:at + 128] = second[k].astype(BF16)

    def step1(i):
        up, vp = i // 3, i % 3
        for t in range(3):
            rhs = MS[i % 3, t]
            for c in range(480 // CHUNK1):
                lo = CHUNK1 * c
                lhs = jnp.concatenate([L2[t, lo:lo + CHUNK1, :], L2[t + 1, lo:lo + CHUNK1, :]], axis=1)
                o = jnp.dot(lhs, rhs, preferred_element_type=F32)
                for k in range(CHUNK1 // 40):
                    q = (CHUNK1 // 40) * c + k
                    for h in range(2):
                        w = jnp.concatenate([o[40 * k:40 * k + 40, 256 * h:256 * h + 128],
                                             o[40 * k:40 * k + 40, 256 * h + 128:256 * h + 256]], axis=0)
                        at = (q % 2) * 384 + t * 128
                        W1[q // 2, 2 * vp + h, up * 80:up * 80 + 80, at:at + 128] = w.astype(BF16)

    boundary(0)
    for i in range(9):
        if i < 8:
            boundary(i + 1)
        step1(i)

    def do2(qp):
        for vp in range(3):
            oa = jnp.dot(KB2[...], W1[qp, 2 * vp], preferred_element_type=F32)
            ob = jnp.dot(KB2[...], W1[qp, 2 * vp + 1], preferred_element_type=F32)
            for g in range(18):
                t = jnp.concatenate([oa[24 * g:24 * g + 24], ob[24 * g:24 * g + 24]], axis=0)
                W2[qp % 2, g, 48 * vp:48 * vp + 48, :] = t.astype(BF16)

    def do3(qp):
        for g in range(18):
            d, rp = g // 3, g % 3
            o = jnp.dot(KB3[:, 0:144], W2[qp % 2, g], preferred_element_type=F32)
            for i in range(12):
                at = ((2 * rp + i // 6) * 6 + i % 6) * 128
                row = qp * 96 + d * 16
                for t in range(3):
                    w = jnp.concatenate([o[8 * i:8 * i + 8, 128 * t:128 * t + 128],
                                         o[8 * i:8 * i + 8, 384 + 128 * t:512 + 128 * t]], axis=0)
                    W3[t, row:row + 16, at:at + 128] = w.astype(BF16)

    def right(r_range):
        right_diff = column(rows[3:4, :])[:96, :96] - qbn[:, :96]
        ahead_row = rows[5:6, :]
        for r in r_range:
            for s in range(6):
                keep = right_diff == ahead_row[:, r:r + 1] - ahead_row[:, s:s + 1]
                t = jnp.concatenate([RB[0, r, s], RB[1, r, s]], axis=0).astype(F32)
                first, second = lane_parts(jnp.where(keep, t, 0.0))
                at = (r * 6 + s) * 128
                for k in range(3):
                    RS[k, 0:96, at:at + 128] = first[k].astype(BF16)
                    RS[k, 128:224, at:at + 128] = second[k].astype(BF16)

    do2(0)
    for qp in range(1, 6):
        if qp == FORWARD_AT:
            right_send.wait_recv()
            right_forward.start()
        if qp == FORWARD_AT + 1:
            right_forward.wait_recv()
            right(range(0, 3))
        if qp == FORWARD_AT + 2:
            right(range(3, 6))
        do2(qp)
        do3(qp - 1)
    do3(5)

    for t in range(3):
        O4[t] = lax.dot_general(W3[t], RS[t], (((1,), (1,)), ((), ())), preferred_element_type=F32)
    acc = jnp.zeros((8, 96), F32)
    for qp in range(6):
        for d in range(6):
            for h in range(2):
                row = qp * 96 + d * 16 + h * 8
                o = [O4[t, row:row + 8, :] for t in range(3)]
                parts = [o[0][:, 0:96], o[0][:, 128:224] + o[1][:, 0:96],
                         o[1][:, 128:224] + o[2][:, 0:96], o[2][:, 128:224]]
                for k in range(4):
                    at = (8 * qp + 4 * h + k) * 48 + d * 8
                    IMG[at:at + 8, 0:96] = parts[k]
                    acc = acc + parts[k] * parts[k]
    mine = jnp.sum(jnp.sum(acc, axis=0, keepdims=True), axis=1, keepdims=True)
    own = SA.at[sec, pl.ds(plane, 1), :]
    own[...] = jnp.broadcast_to(mine, (1, 128))
    plane_sends = [remote(own, own, asend.at[2 * k + f], arecv.at[2 * k + f], plane_peer(k, f))
                   for k in range(plane_n) for f in range(2) if k + f > 0]
    for c in plane_sends:
        c.start()
    plane_sends[0].wait_recv()

    meansq = (SA[0, pl.ds(plane, 1), :] + SA[1, pl.ds(plane, 1), :]) / 331776.0
    scale = lax.rsqrt(meansq + 1e-06)
    for d in range(6):
        for e in range(6):
            t = IMG[pl.ds(d * 8 + e, 48, stride=48), 0:96]
            OUT[d, e] = (t * scale[:, 0:96]).astype(BF16)
    out_copy = pltpu.make_async_copy(OUT, out_h, osem)
    out_copy.start()

    for c in plane_sends[1:]:
        c.wait_recv()
    logs = 0.5 * jnp.log((SA[0] + SA[1]) / 331776.0 + 1e-06)
    SB[pl.ds(z, 1), :] = jnp.sum(logs, axis=0, keepdims=True)
    line = SB.at[pl.ds(z, 1), :]
    line_sends = [remote(line, line, bsend.at[k], brecv.at[k], line_peer(k)) for k in range(1, nz)]
    for c in line_sends:
        c.start()
    for c in line_sends:
        c.wait_recv()
    log_out[...] = jnp.sum(SB[...], axis=0, keepdims=True) / float(count)

    for c in charges + [mps_send, right_send, right_forward] + plane_sends + line_sends:
        c.wait_send()
    out_copy.wait()


def local(sizes, mps, ket, left_proj, right_proj, bond_charge, new_charge, link_charge, vert_charge):
    nx, nz, ny, _ = sizes
    mps_v = mps[0].transpose(1, 2, 0, 3)
    left_v = left_proj[0].transpose(2, 3, 0, 1)
    right_v = right_proj[0].transpose(1, 2, 3, 0)
    ket_v = ket.transpose(0, 1, 2, 3, 5, 4).reshape(432, 6)
    vm = pl.BlockSpec(memory_space=pltpu.VMEM)
    hbm = pl.BlockSpec(memory_space=pl.ANY)
    dma = pltpu.SemaphoreType.DMA
    out, log_row = pl.pallas_call(
        lambda *refs: kernel(sizes, *refs),
        out_shape=(jax.ShapeDtypeStruct((6, 6, 48, 96), BF16), jax.ShapeDtypeStruct((1, 128), F32)),
        in_specs=[hbm] * 10,
        out_specs=(hbm, vm),
        scratch_shapes=[
            pltpu.VMEM((8, 128), I32),
            pltpu.VMEM((1, 96), I32), pltpu.VMEM((1, 96), I32), pltpu.VMEM((1, 6), I32), pltpu.VMEM((1, 2, 6), I32),
            pltpu.VMEM((1, 96), I32), pltpu.VMEM((1, 96), I32), pltpu.VMEM((1, 6), I32),
            pltpu.SMEM((1, 6), I32), pltpu.SMEM((1, 2, 6), I32),
            pltpu.VMEM((992, 128), BF16), pltpu.VMEM((672, 256), BF16),
            pltpu.VMEM((432, 6), BF16), pltpu.VMEM((432, 128), F32),
            pltpu.VMEM((6, 6, 48, 96), BF16),
            pltpu.VMEM((2, 6, 6, 48, 96), BF16), pltpu.VMEM((2, 6, 6, 48, 96), BF16),
            pltpu.VMEM((1728, 128), F32), pltpu.VMEM((4, 480, 128), F32), pltpu.VMEM((4, 480, 128), BF16),
            pltpu.VMEM((3, 3, 256, 512), BF16), pltpu.VMEM((3, 256, 4608), BF16),
            pltpu.VMEM((48, 128), BF16), pltpu.VMEM((432, 256), BF16), pltpu.VMEM((96, 256), BF16),
            pltpu.VMEM((6, 6, 256, 768), BF16), pltpu.VMEM((2, 18, 144, 768), BF16),
            pltpu.VMEM((3, 576, 4608), BF16), pltpu.VMEM((3, 576, 256), F32), pltpu.VMEM((2304, 128), F32),
            pltpu.VMEM((6, 6, 48, 96), BF16),
            pltpu.VMEM((2, nx * ny, 128), F32), pltpu.VMEM((nz, 128), F32),
            dma((11,)), dma((3,)), dma((3,)), dma(()), dma(()), dma(()), dma(()), dma(()), dma(()),
            dma((2 * nx * ny,)), dma((2 * nx * ny,)), dma((nz,)), dma((nz,)), dma(())],
        compiler_params=pltpu.CompilerParams(
            vmem_limit_bytes=VMEM_LIMIT, collective_id=0, has_side_effects=True),
    )(bond_charge, new_charge, link_charge, vert_charge, *operator_tables(), ket_v, mps_v, left_v, right_v)
    return out.transpose(2, 0, 1, 3)[None], log_row[0, 0]


def solution(mesh):
    if mesh.shape["col"] == 128:
        sizes = (4, 8, 4, mesh.shape["sec"])
    else:
        sizes = (2, mesh.shape["col"] // 4, 2, mesh.shape["sec"])
    torus = Mesh(mesh.devices.reshape(sizes), (*COL, "sec"))
    in_specs = (
        P(COL, "sec", None, None, None),
        P(COL, None, None, None, None, None),
        P(COL, "sec", None, None, None),
        P(COL, None, None, None, "sec"),
        P(COL, None),
        P(COL, None),
        P(COL, None),
        P(COL, None, None),
    )
    out_specs = (P(COL, "sec", None, None, None), P())
    return jax.shard_map(lambda *a: local(sizes, *a), mesh=torus, in_specs=in_specs, out_specs=out_specs,
                         check_vma=False)
```

```python
import numpy as np

import jax
import jax.numpy as jnp
from jax import lax
from jax.experimental import pallas as pl
from jax.experimental.pallas import tpu as pltpu
from jax.sharding import Mesh
from jax.sharding import PartitionSpec as P

COL = ("col_0", "col_1", "col_2")
F32, BF16, I32 = jnp.float32, jnp.bfloat16, jnp.int32
MESH = pl.DeviceIdType.MESH
FORWARD_AT = 4
CHUNK1 = 480
VMEM_LIMIT = 67_043_328


def operator_tables():
    e2 = np.zeros((432, 128), np.float32)
    f2 = np.zeros((48, 256), np.float32)
    rows_m = np.full(432, -1)
    cols_m = np.full(256, -2)
    hd = np.zeros((128, 128), np.float32)
    hr = np.zeros((128, 128), np.float32)
    hp = np.zeros((16, 128), np.float32)
    for d in range(6):
        for r in range(6):
            for p in range(2):
                lane = (2 * d + p) * 8 + r
                hd[d, lane] = 1
                hr[r, lane] = 1
                hp[:, lane] = p
                for m in range(6):
                    row = ((r * 6 + d) * 6 + m) * 2 + p
                    e2[row, lane] = 1
                    rows_m[row] = m
    gu = np.zeros((48, 128), np.float32)
    gl = np.zeros((48, 128), np.float32)
    for u in range(6):
        for l in range(6):
            gu[u * 6 + l, u] = 1
            gl[u * 6 + l, l] = 1
            for m in range(6):
                f2[u * 6 + l, u * 40 + l * 6 + m] = 1
                cols_m[u * 40 + l * 6 + m] = m
    k2 = rows_m[:, None] == cols_m[None, :]
    e3 = np.zeros((2, 80, 128), np.float32)
    f3 = np.zeros((2, 48, 256), np.float32)
    rows_d = np.full(80, -1)
    cols_d = np.full(256, -2)
    for d in range(2):
        for s in range(6):
            for e in range(6):
                row = (s * 2 + d) * 6 + e
                rows_d[row] = d
                for p in range(2):
                    e3[p, row, (2 * e + p) * 8 + s] = 1
        for v in range(6):
            for m in range(6):
                for p in range(2):
                    col = v * 24 + d * 12 + m * 2 + p
                    cols_d[col] = d
                    f3[p, v * 6 + m, col] = 1
    k3 = rows_d[:, None] == cols_d[None, :]
    narrow = np.concatenate([e2, e3.reshape(160, 128), hd, hr, gu, gl, hp])
    wide = np.concatenate([f2, k2, f3.reshape(96, 256), k3])
    return jnp.asarray(narrow, BF16), jnp.asarray(wide, BF16)


def column(row):
    return jnp.transpose(jnp.broadcast_to(row, (128, 128)))


def lane_parts(t):
    lane = lax.broadcasted_iota(I32, (96, 128), 1)
    t = jnp.concatenate([t, jnp.zeros((96, 32), F32)], axis=1)
    r32, r64, r96 = (pltpu.roll(t, n, axis=1) for n in (32, 64, 96))
    first = [t, jnp.where(lane < 64, r96, 0.0), jnp.where(lane < 32, r64, 0.0)]
    second = [jnp.where(lane >= 96, r96, 0.0), jnp.where(lane >= 64, r64, 0.0), jnp.where(lane >= 32, r32, 0.0)]
    return first, second


def kernel(sizes, bond, fresh, link, vert, narrow_h, wide_h, ket_h, mps_h, left_h, right_h, out_h, log_out,
           rows, bond_v, fresh_v, link_v, vert_v, bond_n, fresh_n, link_n, link_s, vert_s,
           narrow, wide, KH, KF, left_v, MB, RB, LF, L2F, L2, MS, RS, KM, KB2, KB3, W1, W2, W3, O4, IMG, OUT,
           SA, SB,
           lsem, csend, crecv, msend, mrecv, rsend, rrecv, fsend, frecv, asend, arecv, bsend, brecv, osem):
    nx, nz, ny, _ = sizes
    x, z, y = lax.axis_index("col_0"), lax.axis_index("col_1"), lax.axis_index("col_2")
    sec = lax.axis_index("sec")
    other = 1 - sec
    count = nx * nz * ny
    site = (x * nz + z) * ny + y

    def place(j):
        return {"col_0": lax.div(j, nz * ny), "col_1": lax.rem(lax.div(j, ny), nz), "col_2": lax.rem(j, ny)}

    before = place(lax.rem(site + count - 1, count))
    after = place(lax.rem(site + 1, count))
    partner = {"sec": other}
    plane = x * ny + y

    def plane_peer(dx, dy, flip):
        return {"col_0": lax.rem(x + dx, nx), "col_2": lax.rem(y + dy, ny), "sec": other if flip else sec}

    offsets = [(dx, dy, f) for dx in range(nx) for dy in range(ny) for f in range(2) if dx + dy + f > 0]
    offsets.sort(key=lambda o: -min(o[0], nx - o[0]) - min(o[1], ny - o[1]))
    offsets.remove((0, 0, 1))
    offsets = [(0, 0, 1)] + offsets
    line_offsets = sorted(range(1, nz), key=lambda k: -min(k, nz - k))

    def line_peer(k):
        return {"col_1": lax.rem(z + k, nz)}

    barrier = pltpu.get_barrier_semaphore()
    peers = [line_peer(k) for k in line_offsets] + [plane_peer(*o) for o in offsets] + [before, after]
    for peer in peers:
        pl.semaphore_signal(barrier, inc=1, device_id=peer, device_id_type=MESH)

    fetched = [pltpu.make_async_copy(src, dst, lsem.at[i]) for i, (src, dst) in enumerate([
        (link, link_s), (bond, bond_v), (fresh, fresh_v), (left_h, left_v), (link, link_v), (mps_h, MB.at[sec]),
        (vert, vert_s), (vert, vert_v), (ket_h, KH), (narrow_h, narrow), (wide_h, wide)])]
    for c in fetched:
        c.start()

    rows[...] = jnp.zeros_like(rows)
    LF[...] = jnp.zeros_like(LF)
    L2F[...] = jnp.zeros_like(L2F)
    MS[:, :, 96:128, :] = jnp.zeros((3, 3, 32, 512), BF16)
    MS[:, :, 224:256, :] = jnp.zeros((3, 3, 32, 512), BF16)
    KF[...] = jnp.zeros_like(KF)
    KM[...] = jnp.zeros_like(KM)

    for c in fetched[:4]:
        c.wait()
    rows[0:1, 0:96] = bond_v[...]
    rows[1:2, 0:96] = fresh_v[...]
    qb = rows[0:1, :]
    col_qb = column(qb)
    col_fresh = column(rows[1:2, :])
    fresh_half = jnp.where(sec == 0, col_fresh[0:48, :], col_fresh[48:96, :])
    left_diff = fresh_half[:, :96] - qb[:, :96]
    for l in range(6):
        for m in range(6):
            keep = left_diff == link_s[0, l] - link_s[0, m]
            LF[pl.ds((l * 6 + m) * 48, 48), 0:96] = jnp.where(keep, left_v[l, m].astype(F32), 0.0)

    for c in fetched[4:6]:
        c.wait()
    pl.semaphore_wait(barrier, len(peers))

    def remote(src, dst, send, recv, peer):
        return pltpu.make_async_remote_copy(src_ref=src, dst_ref=dst, send_sem=send, recv_sem=recv,
                                            device_id=peer, device_id_type=MESH)

    charges = [remote(bond_v, bond_n, csend.at[0], crecv.at[0], before),
               remote(link_v, link_n, csend.at[1], crecv.at[1], before),
               remote(fresh_v, fresh_n, csend.at[2], crecv.at[2], before)]
    for c in charges:
        c.start()
    mps_send = remote(MB.at[sec], MB.at[sec], msend, mrecv, partner)
    mps_send.start()
    right_send = remote(right_h, RB.at[sec], rsend, rrecv, before)
    right_send.start()
    right_forward = remote(RB.at[sec], RB.at[sec], fsend, frecv, partner)

    for i in range(48):
        L2F[i % 4, pl.ds(40 * (i // 4), 36), :] = LF[pl.ds(i, 36, stride=48), :]
    L2[...] = L2F[...].astype(BF16)
    W1[:, :, 240:256, :] = jnp.zeros((6, 6, 16, 768), BF16)
    for c in fetched[6:]:
        c.wait()
    KF[:, 0:6] = KH[...].astype(F32)
    ket = None
    for i in range(12):
        part = KF[pl.ds(i, 36, stride=12), :]
        part = part if i == 0 else pltpu.roll(part, 8 * i, axis=1)
        ket = part if ket is None else ket + part

    for c in charges:
        c.wait_recv()
    rows[2:3, 0:96] = bond_n[...]
    rows[3:4, 0:96] = fresh_n[...]
    rows[4:5, 0:6] = link_v[...]
    rows[5:6, 0:6] = link_n[...]
    rows[6:8, 0:6] = vert_v[0]
    qbn = rows[2:3, :]

    def operators():
        charge_rows = rows[...].astype(F32)
        ket_rows = jnp.sum(narrow[848:896, :].astype(F32) * charge_rows[6:7, :]
                           + narrow[896:944, :].astype(F32) * charge_rows[4:5, :], axis=1, keepdims=True)
        lower = jnp.broadcast_to(charge_rows[7:8, :], (16, 128)).astype(BF16)
        ahead = jnp.broadcast_to(charge_rows[5:6, :], (16, 128)).astype(BF16)
        ket_cols = (jnp.dot(lower, narrow[592:720, :], preferred_element_type=F32)
                    + jnp.dot(ahead, narrow[720:848, :], preferred_element_type=F32)
                    + narrow[944:960, :].astype(F32))[0:1, :]
        keep = jnp.abs(ket_rows[0:36] - ket_cols) < 0.5
        KM[0:36, :] = jnp.where(keep, ket, 0.0).astype(BF16)
        spread = lax.dot_general(narrow[0:432, :], KM[...], (((1,), (1,)), ((), ())), preferred_element_type=F32)
        KB2[...] = (jnp.dot(spread.astype(BF16), wide[0:48, :], preferred_element_type=F32)
                    * wide[48:480, :].astype(F32)).astype(BF16)
        total = None
        for p in range(2):
            spread = lax.dot_general(narrow[432 + 80 * p:512 + 80 * p, :], KM[...], (((1,), (1,)), ((), ())),
                                     preferred_element_type=F32)
            part = jnp.dot(spread.astype(BF16), wide[480 + 48 * p:528 + 48 * p, :], preferred_element_type=F32)
            total = part if total is None else total + part
        KB3[...] = (total * wide[576:656, :].astype(F32)).astype(BF16)

    bond_diff = qbn[:, :96] - col_qb[:96, :96]
    mps_send.wait_recv()

    def boundary(i):
        up, vp = i // 3, i % 3
        for v in (2 * vp, 2 * vp + 1):
            for u in (2 * up, 2 * up + 1):
                keep = bond_diff == vert_s[0, 0, u] - vert_s[0, 0, v]
                t = jnp.concatenate([MB[0, u, v], MB[1, u, v]], axis=0).astype(F32)
                first, second = lane_parts(jnp.where(keep, t, 0.0))
                at = ((u % 2) + 2 * (v % 2)) * 128
                for k in range(3):
                    MS[i % 3, k, 0:96, at:at + 128] = first[k].astype(BF16)
                    MS[i % 3, k, 128:224, at:at + 128] = second[k].astype(BF16)

    def step1(i):
        up, vp = i // 3, i % 3
        for t in range(3):
            rhs = MS[i % 3, t]
            for c in range(480 // CHUNK1):
                lo = CHUNK1 * c
                lhs = jnp.concatenate([L2[t, lo:lo + CHUNK1, :], L2[t + 1, lo:lo + CHUNK1, :]], axis=1)
                o = jnp.dot(lhs, rhs, preferred_element_type=F32)
                for k in range(CHUNK1 // 40):
                    q = (CHUNK1 // 40) * c + k
                    for h in range(2):
                        w = jnp.concatenate([o[40 * k:40 * k + 40, 256 * h:256 * h + 128],
                                             o[40 * k:40 * k + 40, 256 * h + 128:256 * h + 256]], axis=0)
                        at = (q % 2) * 384 + t * 128
                        W1[q // 2, 2 * vp + h, up * 80:up * 80 + 80, at:at + 128] = w.astype(BF16)

    boundary(0)
    operators()
    for i in range(9):
        if i < 8:
            boundary(i + 1)
        step1(i)

    def do2(qp):
        for vp in range(3):
            oa = jnp.dot(KB2[...], W1[qp, 2 * vp], preferred_element_type=F32)
            ob = jnp.dot(KB2[...], W1[qp, 2 * vp + 1], preferred_element_type=F32)
            for g in range(18):
                t = jnp.concatenate([oa[24 * g:24 * g + 24], ob[24 * g:24 * g + 24]], axis=0)
                W2[qp % 2, g, 48 * vp:48 * vp + 48, :] = t.astype(BF16)

    def do3(qp):
        for g in range(18):
            r, dp = g // 3, g % 3
            o = jnp.dot(KB3[0:72, 0:144], W2[qp % 2, g], preferred_element_type=F32)
            row = qp * 72 + dp * 24
            for i in range(6):
                at = (r * 6 + i) * 128
                for t in range(3):
                    w = jnp.concatenate([o[12 * i:12 * i + 12, 128 * t:128 * t + 128],
                                         o[12 * i:12 * i + 12, 384 + 128 * t:512 + 128 * t]], axis=0)
                    W3[t, row:row + 24, at:at + 128] = w.astype(BF16)

    def right(r_range):
        right_diff = column(rows[3:4, :])[:96, :96] - qbn[:, :96]
        ahead_row = rows[5:6, :]
        for r in r_range:
            for s in range(6):
                keep = right_diff == ahead_row[:, r:r + 1] - ahead_row[:, s:s + 1]
                t = jnp.concatenate([RB[0, r, s], RB[1, r, s]], axis=0).astype(F32)
                first, second = lane_parts(jnp.where(keep, t, 0.0))
                at = (r * 6 + s) * 128
                for k in range(3):
                    RS[k, 0:96, at:at + 128] = first[k].astype(BF16)
                    RS[k, 128:224, at:at + 128] = second[k].astype(BF16)

    do2(0)
    for qp in range(1, 6):
        if qp == FORWARD_AT:
            right_send.wait_recv()
            right_forward.start()
        do2(qp)
        do3(qp - 1)
    right_forward.wait_recv()
    right(range(6))
    do3(5)

    for t in range(3):
        O4[t] = lax.dot_general(W3[t], RS[t], (((1,), (1,)), ((), ())), preferred_element_type=F32)
    acc = jnp.zeros((12, 96), F32)
    for qp in range(6):
        for dp in range(3):
            for h in range(2):
                row = qp * 72 + dp * 24 + h * 12
                o = [O4[t, row:row + 12, :] for t in range(3)]
                parts = [o[0][:, 0:96], o[0][:, 128:224] + o[1][:, 0:96],
                         o[1][:, 128:224] + o[2][:, 0:96], o[2][:, 128:224]]
                for k in range(4):
                    at = (8 * qp + 4 * h + k) * 36 + dp * 12
                    IMG[at:at + 12, 0:96] = parts[k]
                    acc = acc + parts[k] * parts[k]
    mine = jnp.sum(jnp.sum(acc, axis=0, keepdims=True), axis=1, keepdims=True)
    own = SA.at[sec, pl.ds(plane, 1), :]
    own[...] = jnp.broadcast_to(mine, (1, 128))
    plane_sends = []
    for dx, dy, f in offsets:
        i = 2 * (dx * ny + dy) + f
        plane_sends.append(remote(own, own, asend.at[i], arecv.at[i], plane_peer(dx, dy, f)))
    for c in plane_sends:
        c.start()
    plane_sends[0].wait_recv()

    meansq = (SA[0, pl.ds(plane, 1), :] + SA[1, pl.ds(plane, 1), :]) / 331776.0
    scale = lax.rsqrt(meansq + 1e-06)
    for d in range(6):
        for e in range(6):
            t = IMG[pl.ds(d * 6 + e, 48, stride=36), 0:96]
            OUT[d, e] = (t * scale[:, 0:96]).astype(BF16)
    out_copy = pltpu.make_async_copy(OUT, out_h, osem)
    out_copy.start()

    for c in plane_sends[1:]:
        c.wait_recv()
    logs = 0.5 * jnp.log((SA[0] + SA[1]) / 331776.0 + 1e-06)
    SB[pl.ds(z, 1), :] = jnp.sum(logs, axis=0, keepdims=True)
    line = SB.at[pl.ds(z, 1), :]
    line_sends = [remote(line, line, bsend.at[k], brecv.at[k], line_peer(k)) for k in line_offsets]
    for c in line_sends:
        c.start()
    for c in line_sends:
        c.wait_recv()
    log_out[...] = jnp.sum(SB[...], axis=0, keepdims=True) / float(count)

    for c in charges + [mps_send, right_send, right_forward] + plane_sends + line_sends:
        c.wait_send()
    out_copy.wait()


def local(sizes, mps, ket, left_proj, right_proj, bond_charge, new_charge, link_charge, vert_charge):
    nx, nz, ny, _ = sizes
    mps_v = mps[0].transpose(1, 2, 0, 3)
    left_v = left_proj[0].transpose(2, 3, 0, 1)
    right_v = right_proj[0].transpose(1, 2, 3, 0)
    ket_v = ket.transpose(0, 1, 2, 3, 5, 4).reshape(432, 6)
    vm = pl.BlockSpec(memory_space=pltpu.VMEM)
    hbm = pl.BlockSpec(memory_space=pl.ANY)
    dma = pltpu.SemaphoreType.DMA
    out, log_row = pl.pallas_call(
        lambda *refs: kernel(sizes, *refs),
        out_shape=(jax.ShapeDtypeStruct((6, 6, 48, 96), BF16), jax.ShapeDtypeStruct((1, 128), F32)),
        in_specs=[hbm] * 10,
        out_specs=(hbm, vm),
        scratch_shapes=[
            pltpu.VMEM((8, 128), I32),
            pltpu.VMEM((1, 96), I32), pltpu.VMEM((1, 96), I32), pltpu.VMEM((1, 6), I32), pltpu.VMEM((1, 2, 6), I32),
            pltpu.VMEM((1, 96), I32), pltpu.VMEM((1, 96), I32), pltpu.VMEM((1, 6), I32),
            pltpu.SMEM((1, 6), I32), pltpu.SMEM((1, 2, 6), I32),
            pltpu.VMEM((960, 128), BF16), pltpu.VMEM((656, 256), BF16),
            pltpu.VMEM((432, 6), BF16), pltpu.VMEM((432, 128), F32),
            pltpu.VMEM((6, 6, 48, 96), BF16),
            pltpu.VMEM((2, 6, 6, 48, 96), BF16), pltpu.VMEM((2, 6, 6, 48, 96), BF16),
            pltpu.VMEM((1728, 128), F32), pltpu.VMEM((4, 480, 128), F32), pltpu.VMEM((4, 480, 128), BF16),
            pltpu.VMEM((3, 3, 256, 512), BF16), pltpu.VMEM((3, 256, 4608), BF16),
            pltpu.VMEM((48, 128), BF16), pltpu.VMEM((432, 256), BF16), pltpu.VMEM((80, 256), BF16),
            pltpu.VMEM((6, 6, 256, 768), BF16), pltpu.VMEM((2, 18, 144, 768), BF16),
            pltpu.VMEM((3, 432, 4608), BF16), pltpu.VMEM((3, 432, 256), F32), pltpu.VMEM((1728, 128), F32),
            pltpu.VMEM((6, 6, 48, 96), BF16),
            pltpu.VMEM((2, nx * ny, 128), F32), pltpu.VMEM((nz, 128), F32),
            dma((11,)), dma((3,)), dma((3,)), dma(()), dma(()), dma(()), dma(()), dma(()), dma(()),
            dma((2 * nx * ny,)), dma((2 * nx * ny,)), dma((nz,)), dma((nz,)), dma(())],
        compiler_params=pltpu.CompilerParams(
            vmem_limit_bytes=VMEM_LIMIT, collective_id=0, has_side_effects=True),
    )(bond_charge, new_charge, link_charge, vert_charge, *operator_tables(), ket_v, mps_v, left_v, right_v)
    return out.transpose(2, 0, 1, 3)[None], log_row[0, 0]


def solution(mesh):
    if mesh.shape["col"] == 128:
        sizes = (4, 8, 4, mesh.shape["sec"])
    else:
        sizes = (2, mesh.shape["col"] // 4, 2, mesh.shape["sec"])
    torus = Mesh(mesh.devices.reshape(sizes), (*COL, "sec"))
    in_specs = (
        P(COL, "sec", None, None, None),
        P(COL, None, None, None, None, None),
        P(COL, "sec", None, None, None),
        P(COL, None, None, None, "sec"),
        P(COL, None),
        P(COL, None),
        P(COL, None),
        P(COL, None, None),
    )
    out_specs = (P(COL, "sec", None, None, None), P())
    return jax.shard_map(lambda *a: local(sizes, *a), mesh=torus, in_specs=in_specs, out_specs=out_specs,
                         check_vma=False)
```

```python
import numpy as np

import jax
import jax.numpy as jnp
from jax import lax
from jax.experimental import pallas as pl
from jax.experimental.pallas import tpu as pltpu
from jax.sharding import Mesh
from jax.sharding import PartitionSpec as P

COL = ("col_0", "col_1", "col_2")
F32, BF16, I32 = jnp.float32, jnp.bfloat16, jnp.int32
MESH = pl.DeviceIdType.MESH
FORWARD_AT = 4
CHUNK1 = 480
VMEM_LIMIT = 60_000_000


def operator_tables():
    e2 = np.zeros((432, 128), np.float32)
    f2 = np.zeros((48, 256), np.float32)
    rows_m = np.full(432, -1)
    cols_m = np.full(256, -2)
    hd = np.zeros((128, 128), np.float32)
    hr = np.zeros((128, 128), np.float32)
    hp = np.zeros((16, 128), np.float32)
    for d in range(6):
        for r in range(6):
            for p in range(2):
                lane = (2 * d + p) * 8 + r
                hd[d, lane] = 1
                hr[r, lane] = 1
                hp[:, lane] = p
                for m in range(6):
                    row = ((r * 6 + d) * 6 + m) * 2 + p
                    e2[row, lane] = 1
                    rows_m[row] = m
    gu = np.zeros((48, 128), np.float32)
    gl = np.zeros((48, 128), np.float32)
    for u in range(6):
        for l in range(6):
            gu[u * 6 + l, u] = 1
            gl[u * 6 + l, l] = 1
            for m in range(6):
                f2[u * 6 + l, u * 40 + l * 6 + m] = 1
                cols_m[u * 40 + l * 6 + m] = m
    k2 = rows_m[:, None] == cols_m[None, :]
    e3 = np.zeros((2, 80, 128), np.float32)
    f3 = np.zeros((2, 48, 256), np.float32)
    rows_d = np.full(80, -1)
    cols_d = np.full(256, -2)
    for d in range(2):
        for s in range(6):
            for e in range(6):
                row = (s * 2 + d) * 6 + e
                rows_d[row] = d
                for p in range(2):
                    e3[p, row, (2 * e + p) * 8 + s] = 1
        for v in range(6):
            for m in range(6):
                for p in range(2):
                    col = v * 24 + d * 12 + m * 2 + p
                    cols_d[col] = d
                    f3[p, v * 6 + m, col] = 1
    k3 = rows_d[:, None] == cols_d[None, :]
    narrow = np.concatenate([e2, e3.reshape(160, 128), hd, hr, gu, gl, hp])
    wide = np.concatenate([f2, k2, f3.reshape(96, 256), k3])
    return jnp.asarray(narrow, BF16), jnp.asarray(wide, BF16)


def column(row):
    return jnp.transpose(jnp.broadcast_to(row, (128, 128)))


def lane_parts(t):
    lane = lax.broadcasted_iota(I32, (96, 128), 1)
    t = jnp.concatenate([t, jnp.zeros((96, 32), F32)], axis=1)
    r32, r64, r96 = (pltpu.roll(t, n, axis=1) for n in (32, 64, 96))
    first = [t, jnp.where(lane < 64, r96, 0.0), jnp.where(lane < 32, r64, 0.0)]
    second = [jnp.where(lane >= 96, r96, 0.0), jnp.where(lane >= 64, r64, 0.0), jnp.where(lane >= 32, r32, 0.0)]
    return first, second


def kernel(sizes, bond, fresh, link, vert, narrow_h, wide_h, ket_h, mps_h, left_h, right_h, out_h, log_out,
           rows, bond_v, fresh_v, link_v, vert_v, bond_n, fresh_n, link_n, link_s, vert_s,
           narrow, wide, KH, KF, left_v, MB, RB, LF, L2F, L2, MS, RS, KM, KB2, KB3, W1, W2, W3, O4, IMG,
           SA, SB,
           lsem, csend, crecv, msend, mrecv, rsend, rrecv, fsend, frecv, asend, arecv, bsend, brecv):
    nx, nz, ny, _ = sizes
    x, z, y = lax.axis_index("col_0"), lax.axis_index("col_1"), lax.axis_index("col_2")
    sec = lax.axis_index("sec")
    other = 1 - sec
    count = nx * nz * ny
    site = (x * nz + z) * ny + y

    def place(j):
        return {"col_0": lax.div(j, nz * ny), "col_1": lax.rem(lax.div(j, ny), nz), "col_2": lax.rem(j, ny)}

    before = place(lax.rem(site + count - 1, count))
    after = place(lax.rem(site + 1, count))
    partner = {"sec": other}
    plane = x * ny + y

    def plane_peer(dx, dy, flip):
        return {"col_0": lax.rem(x + dx, nx), "col_2": lax.rem(y + dy, ny), "sec": other if flip else sec}

    offsets = [(dx, dy, f) for dx in range(nx) for dy in range(ny) for f in range(2) if dx + dy + f > 0]
    offsets.sort(key=lambda o: -min(o[0], nx - o[0]) - min(o[1], ny - o[1]))
    offsets.remove((0, 0, 1))
    offsets = [(0, 0, 1)] + offsets
    line_offsets = sorted(range(1, nz), key=lambda k: -min(k, nz - k))

    def line_peer(k):
        return {"col_1": lax.rem(z + k, nz)}

    barrier = pltpu.get_barrier_semaphore()
    peers = [line_peer(k) for k in line_offsets] + [plane_peer(*o) for o in offsets] + [before, after]
    for peer in peers:
        pl.semaphore_signal(barrier, inc=1, device_id=peer, device_id_type=MESH)

    fetched = [pltpu.make_async_copy(src, dst, lsem.at[i]) for i, (src, dst) in enumerate([
        (link, link_s), (bond, bond_v), (fresh, fresh_v), (left_h, left_v), (link, link_v), (mps_h, MB.at[sec]),
        (vert, vert_s), (vert, vert_v), (ket_h, KH), (narrow_h, narrow), (wide_h, wide)])]
    for c in fetched:
        c.start()

    rows[...] = jnp.zeros_like(rows)
    LF[...] = jnp.zeros_like(LF)
    L2F[...] = jnp.zeros_like(L2F)
    MS[:, :, 96:128, :] = jnp.zeros((3, 3, 32, 512), BF16)
    MS[:, :, 224:256, :] = jnp.zeros((3, 3, 32, 512), BF16)
    KF[...] = jnp.zeros_like(KF)
    KM[...] = jnp.zeros_like(KM)

    for c in fetched[:4]:
        c.wait()
    rows[0:1, 0:96] = bond_v[...]
    rows[1:2, 0:96] = fresh_v[...]
    qb = rows[0:1, :]
    col_qb = column(qb)
    col_fresh = column(rows[1:2, :])
    fresh_half = jnp.where(sec == 0, col_fresh[0:48, :], col_fresh[48:96, :])
    left_diff = fresh_half[:, :96] - qb[:, :96]
    for l in range(6):
        for m in range(6):
            keep = left_diff == link_s[0, l] - link_s[0, m]
            LF[pl.ds((l * 6 + m) * 48, 48), 0:96] = jnp.where(keep, left_v[l, m].astype(F32), 0.0)

    for c in fetched[4:6]:
        c.wait()
    pl.semaphore_wait(barrier, len(peers))

    def remote(src, dst, send, recv, peer):
        return pltpu.make_async_remote_copy(src_ref=src, dst_ref=dst, send_sem=send, recv_sem=recv,
                                            device_id=peer, device_id_type=MESH)

    charges = [remote(bond_v, bond_n, csend.at[0], crecv.at[0], before),
               remote(link_v, link_n, csend.at[1], crecv.at[1], before),
               remote(fresh_v, fresh_n, csend.at[2], crecv.at[2], before)]
    for c in charges:
        c.start()
    mps_send = remote(MB.at[sec], MB.at[sec], msend, mrecv, partner)
    mps_send.start()
    right_send = remote(right_h, RB.at[sec], rsend, rrecv, before)
    right_send.start()
    right_forward = remote(RB.at[sec], RB.at[sec], fsend, frecv, partner)

    for i in range(48):
        L2F[i % 4, pl.ds(40 * (i // 4), 36), :] = LF[pl.ds(i, 36, stride=48), :]
    L2[...] = L2F[...].astype(BF16)
    W1[:, :, 240:256, :] = jnp.zeros((6, 6, 16, 768), BF16)
    for c in fetched[6:]:
        c.wait()
    KF[:, 0:6] = KH[...].astype(F32)
    ket = None
    for i in range(12):
        part = KF[pl.ds(i, 36, stride=12), :]
        part = part if i == 0 else pltpu.roll(part, 8 * i, axis=1)
        ket = part if ket is None else ket + part

    for c in charges:
        c.wait_recv()
    rows[2:3, 0:96] = bond_n[...]
    rows[3:4, 0:96] = fresh_n[...]
    rows[4:5, 0:6] = link_v[...]
    rows[5:6, 0:6] = link_n[...]
    rows[6:8, 0:6] = vert_v[0]
    qbn = rows[2:3, :]

    def operators():
        charge_rows = rows[...].astype(F32)
        ket_rows = jnp.sum(narrow[848:896, :].astype(F32) * charge_rows[6:7, :]
                           + narrow[896:944, :].astype(F32) * charge_rows[4:5, :], axis=1, keepdims=True)
        lower = jnp.broadcast_to(charge_rows[7:8, :], (16, 128)).astype(BF16)
        ahead = jnp.broadcast_to(charge_rows[5:6, :], (16, 128)).astype(BF16)
        ket_cols = (jnp.dot(lower, narrow[592:720, :], preferred_element_type=F32)
                    + jnp.dot(ahead, narrow[720:848, :], preferred_element_type=F32)
                    + narrow[944:960, :].astype(F32))[0:1, :]
        keep = jnp.abs(ket_rows[0:36] - ket_cols) < 0.5
        KM[0:36, :] = jnp.where(keep, ket, 0.0).astype(BF16)
        spread = lax.dot_general(narrow[0:432, :], KM[...], (((1,), (1,)), ((), ())), preferred_element_type=F32)
        KB2[...] = (jnp.dot(spread.astype(BF16), wide[0:48, :], preferred_element_type=F32)
                    * wide[48:480, :].astype(F32)).astype(BF16)
        total = None
        for p in range(2):
            spread = lax.dot_general(narrow[432 + 80 * p:512 + 80 * p, :], KM[...], (((1,), (1,)), ((), ())),
                                     preferred_element_type=F32)
            part = jnp.dot(spread.astype(BF16), wide[480 + 48 * p:528 + 48 * p, :], preferred_element_type=F32)
            total = part if total is None else total + part
        KB3[...] = (total * wide[576:656, :].astype(F32)).astype(BF16)

    bond_diff = qbn[:, :96] - col_qb[:96, :96]
    mps_send.wait_recv()

    def boundary(i):
        up, vp = i // 3, i % 3
        for v in (2 * vp, 2 * vp + 1):
            for u in (2 * up, 2 * up + 1):
                keep = bond_diff == vert_s[0, 0, u] - vert_s[0, 0, v]
                t = jnp.concatenate([MB[0, u, v], MB[1, u, v]], axis=0).astype(F32)
                first, second = lane_parts(jnp.where(keep, t, 0.0))
                at = ((u % 2) + 2 * (v % 2)) * 128
                for k in range(3):
                    MS[i % 3, k, 0:96, at:at + 128] = first[k].astype(BF16)
                    MS[i % 3, k, 128:224, at:at + 128] = second[k].astype(BF16)

    def step1(i):
        up, vp = i // 3, i % 3
        for t in range(3):
            rhs = MS[i % 3, t]
            for c in range(480 // CHUNK1):
                lo = CHUNK1 * c
                lhs = jnp.concatenate([L2[t, lo:lo + CHUNK1, :], L2[t + 1, lo:lo + CHUNK1, :]], axis=1)
                o = jnp.dot(lhs, rhs, preferred_element_type=F32)
                for k in range(CHUNK1 // 40):
                    q = (CHUNK1 // 40) * c + k
                    for h in range(2):
                        w = jnp.concatenate([o[40 * k:40 * k + 40, 256 * h:256 * h + 128],
                                             o[40 * k:40 * k + 40, 256 * h + 128:256 * h + 256]], axis=0)
                        at = (q % 2) * 384 + t * 128
                        W1[q // 2, 2 * vp + h, up * 80:up * 80 + 80, at:at + 128] = w.astype(BF16)

    boundary(0)
    operators()
    for i in range(9):
        if i < 8:
            boundary(i + 1)
        step1(i)

    def do2(qp):
        for vp in range(3):
            oa = jnp.dot(KB2[...], W1[qp, 2 * vp], preferred_element_type=F32)
            ob = jnp.dot(KB2[...], W1[qp, 2 * vp + 1], preferred_element_type=F32)
            for g in range(18):
                t = jnp.concatenate([oa[24 * g:24 * g + 24], ob[24 * g:24 * g + 24]], axis=0)
                W2[qp % 2, g, 48 * vp:48 * vp + 48, :] = t.astype(BF16)

    def do3(qp):
        for g in range(18):
            r, dp = g // 3, g % 3
            o = jnp.dot(KB3[0:72, 0:144], W2[qp % 2, g], preferred_element_type=F32)
            row = qp * 72 + dp * 24
            for i in range(6):
                at = (r * 6 + i) * 128
                for t in range(3):
                    w = jnp.concatenate([o[12 * i:12 * i + 12, 128 * t:128 * t + 128],
                                         o[12 * i:12 * i + 12, 384 + 128 * t:512 + 128 * t]], axis=0)
                    W3[t, row:row + 24, at:at + 128] = w.astype(BF16)

    def right(r_range):
        right_diff = column(rows[3:4, :])[:96, :96] - qbn[:, :96]
        ahead_row = rows[5:6, :]
        for r in r_range:
            for s in range(6):
                keep = right_diff == ahead_row[:, r:r + 1] - ahead_row[:, s:s + 1]
                t = jnp.concatenate([RB[0, r, s], RB[1, r, s]], axis=0).astype(F32)
                first, second = lane_parts(jnp.where(keep, t, 0.0))
                at = (r * 6 + s) * 128
                for k in range(3):
                    RS[k, 0:96, at:at + 128] = first[k].astype(BF16)
                    RS[k, 128:224, at:at + 128] = second[k].astype(BF16)

    do2(0)
    for qp in range(1, 6):
        if qp == FORWARD_AT:
            right_send.wait_recv()
            right_forward.start()
        do2(qp)
        do3(qp - 1)
    right_forward.wait_recv()
    right(range(6))
    do3(5)

    for t in range(3):
        O4[t] = lax.dot_general(W3[t], RS[t], (((1,), (1,)), ((), ())), preferred_element_type=F32)
    acc = jnp.zeros((12, 96), F32)
    for qp in range(6):
        for dp in range(3):
            for h in range(2):
                row = qp * 72 + dp * 24 + h * 12
                o = [O4[t, row:row + 12, :] for t in range(3)]
                parts = [o[0][:, 0:96], o[0][:, 128:224] + o[1][:, 0:96],
                         o[1][:, 128:224] + o[2][:, 0:96], o[2][:, 128:224]]
                for k in range(4):
                    at = (8 * qp + 4 * h + k) * 36 + dp * 12
                    IMG[at:at + 12, 0:96] = parts[k]
                    acc = acc + parts[k] * parts[k]
    mine = jnp.sum(jnp.sum(acc, axis=0, keepdims=True), axis=1, keepdims=True)
    own = SA.at[sec, pl.ds(plane, 1), :]
    own[...] = jnp.broadcast_to(mine, (1, 128))
    plane_sends = []
    for dx, dy, f in offsets:
        i = 2 * (dx * ny + dy) + f
        plane_sends.append(remote(own, own, asend.at[i], arecv.at[i], plane_peer(dx, dy, f)))
    for c in plane_sends:
        c.start()
    plane_sends[0].wait_recv()

    meansq = (SA[0, pl.ds(plane, 1), :] + SA[1, pl.ds(plane, 1), :]) / 331776.0
    scale = lax.rsqrt(meansq + 1e-06)
    for d in range(6):
        for e in range(6):
            t = IMG[pl.ds(d * 6 + e, 48, stride=36), 0:96]
            out_h[d, e] = (t * scale[:, 0:96]).astype(BF16)

    for c in plane_sends[1:]:
        c.wait_recv()
    logs = 0.5 * jnp.log((SA[0] + SA[1]) / 331776.0 + 1e-06)
    SB[pl.ds(z, 1), :] = jnp.sum(logs, axis=0, keepdims=True)
    line = SB.at[pl.ds(z, 1), :]
    line_sends = [remote(line, line, bsend.at[k], brecv.at[k], line_peer(k)) for k in line_offsets]
    for c in line_sends:
        c.start()
    for c in line_sends:
        c.wait_recv()
    log_out[...] = jnp.sum(SB[...], axis=0, keepdims=True) / float(count)

    for c in charges + [mps_send, right_send, right_forward] + plane_sends + line_sends:
        c.wait_send()


def local(sizes, mps, ket, left_proj, right_proj, bond_charge, new_charge, link_charge, vert_charge):
    nx, nz, ny, _ = sizes
    mps_v = mps[0].transpose(1, 2, 0, 3)
    left_v = left_proj[0].transpose(2, 3, 0, 1)
    right_v = right_proj[0].transpose(1, 2, 3, 0)
    ket_v = ket.transpose(0, 1, 2, 3, 5, 4).reshape(432, 6)
    vm = pl.BlockSpec(memory_space=pltpu.VMEM)
    hbm = pl.BlockSpec(memory_space=pl.ANY)
    dma = pltpu.SemaphoreType.DMA
    out, log_row = pl.pallas_call(
        lambda *refs: kernel(sizes, *refs),
        out_shape=(pltpu.VMEM((6, 6, 48, 96), BF16), jax.ShapeDtypeStruct((1, 128), F32)),
        in_specs=[hbm] * 10,
        out_specs=(vm, vm),
        scratch_shapes=[
            pltpu.VMEM((8, 128), I32),
            pltpu.VMEM((1, 96), I32), pltpu.VMEM((1, 96), I32), pltpu.VMEM((1, 6), I32), pltpu.VMEM((1, 2, 6), I32),
            pltpu.VMEM((1, 96), I32), pltpu.VMEM((1, 96), I32), pltpu.VMEM((1, 6), I32),
            pltpu.SMEM((1, 6), I32), pltpu.SMEM((1, 2, 6), I32),
            pltpu.VMEM((960, 128), BF16), pltpu.VMEM((656, 256), BF16),
            pltpu.VMEM((432, 6), BF16), pltpu.VMEM((432, 128), F32),
            pltpu.VMEM((6, 6, 48, 96), BF16),
            pltpu.VMEM((2, 6, 6, 48, 96), BF16), pltpu.VMEM((2, 6, 6, 48, 96), BF16),
            pltpu.VMEM((1728, 128), F32), pltpu.VMEM((4, 480, 128), F32), pltpu.VMEM((4, 480, 128), BF16),
            pltpu.VMEM((3, 3, 256, 512), BF16), pltpu.VMEM((3, 256, 4608), BF16),
            pltpu.VMEM((48, 128), BF16), pltpu.VMEM((432, 256), BF16), pltpu.VMEM((80, 256), BF16),
            pltpu.VMEM((6, 6, 256, 768), BF16), pltpu.VMEM((2, 18, 144, 768), BF16),
            pltpu.VMEM((3, 432, 4608), BF16), pltpu.VMEM((3, 432, 256), F32), pltpu.VMEM((1728, 128), F32),
            pltpu.VMEM((2, nx * ny, 128), F32), pltpu.VMEM((nz, 128), F32),
            dma((11,)), dma((3,)), dma((3,)), dma(()), dma(()), dma(()), dma(()), dma(()), dma(()),
            dma((2 * nx * ny,)), dma((2 * nx * ny,)), dma((nz,)), dma((nz,))],
        compiler_params=pltpu.CompilerParams(
            vmem_limit_bytes=VMEM_LIMIT, collective_id=0, has_side_effects=True),
    )(bond_charge, new_charge, link_charge, vert_charge, *operator_tables(), ket_v, mps_v, left_v, right_v)
    return out.transpose(2, 0, 1, 3)[None], log_row[0, 0]


def solution(mesh):
    if mesh.shape["col"] == 128:
        sizes = (4, 8, 4, mesh.shape["sec"])
    else:
        sizes = (2, mesh.shape["col"] // 4, 2, mesh.shape["sec"])
    torus = Mesh(mesh.devices.reshape(sizes), (*COL, "sec"))
    in_specs = (
        P(COL, "sec", None, None, None),
        P(COL, None, None, None, None, None),
        P(COL, "sec", None, None, None),
        P(COL, None, None, None, "sec"),
        P(COL, None),
        P(COL, None),
        P(COL, None),
        P(COL, None, None),
    )
    out_specs = (P(COL, "sec", None, None, None), P())
    return jax.shard_map(lambda *a: local(sizes, *a), mesh=torus, in_specs=in_specs, out_specs=out_specs,
                         check_vma=False)
```

```python
import numpy as np

import jax
import jax.numpy as jnp
from jax import lax
from jax.experimental import pallas as pl
from jax.experimental.pallas import tpu as pltpu
from jax.sharding import Mesh
from jax.sharding import PartitionSpec as P

COL = ("col_0", "col_1", "col_2")
F32, BF16, I32 = jnp.float32, jnp.bfloat16, jnp.int32
MESH = pl.DeviceIdType.MESH
FORWARD_AT = 4
CHUNK1 = 480
VMEM_LIMIT = 60_000_000


def operator_tables():
    e2 = np.zeros((432, 128), np.float32)
    f2 = np.zeros((48, 256), np.float32)
    rows_m = np.full(432, -1)
    cols_m = np.full(256, -2)
    hd = np.zeros((128, 128), np.float32)
    hr = np.zeros((128, 128), np.float32)
    hp = np.zeros((16, 128), np.float32)
    for d in range(6):
        for r in range(6):
            for p in range(2):
                lane = (2 * d + p) * 8 + r
                hd[d, lane] = 1
                hr[r, lane] = 1
                hp[:, lane] = p
                for m in range(6):
                    row = ((r * 6 + d) * 6 + m) * 2 + p
                    e2[row, lane] = 1
                    rows_m[row] = m
    gu = np.zeros((48, 128), np.float32)
    gl = np.zeros((48, 128), np.float32)
    for u in range(6):
        for l in range(6):
            gu[u * 6 + l, u] = 1
            gl[u * 6 + l, l] = 1
            for m in range(6):
                f2[u * 6 + l, u * 40 + l * 6 + m] = 1
                cols_m[u * 40 + l * 6 + m] = m
    k2 = rows_m[:, None] == cols_m[None, :]
    e3 = np.zeros((2, 80, 128), np.float32)
    f3 = np.zeros((2, 48, 256), np.float32)
    rows_d = np.full(80, -1)
    cols_d = np.full(256, -2)
    for d in range(2):
        for s in range(6):
            for e in range(6):
                row = (s * 2 + d) * 6 + e
                rows_d[row] = d
                for p in range(2):
                    e3[p, row, (2 * e + p) * 8 + s] = 1
        for v in range(6):
            for m in range(6):
                for p in range(2):
                    col = v * 24 + d * 12 + m * 2 + p
                    cols_d[col] = d
                    f3[p, v * 6 + m, col] = 1
    k3 = rows_d[:, None] == cols_d[None, :]
    narrow = np.concatenate([e2, e3.reshape(160, 128), hd, hr, gu, gl, hp])
    wide = np.concatenate([f2, k2, f3.reshape(96, 256), k3])
    return jnp.asarray(narrow, BF16), jnp.asarray(wide, BF16)


def column(row):
    return jnp.transpose(jnp.broadcast_to(row, (128, 128)))


def lane_parts(t):
    lane = lax.broadcasted_iota(I32, (96, 128), 1)
    t = jnp.concatenate([t, jnp.zeros((96, 32), F32)], axis=1)
    r32, r64, r96 = (pltpu.roll(t, n, axis=1) for n in (32, 64, 96))
    first = [t, jnp.where(lane < 64, r96, 0.0), jnp.where(lane < 32, r64, 0.0)]
    second = [jnp.where(lane >= 96, r96, 0.0), jnp.where(lane >= 64, r64, 0.0), jnp.where(lane >= 32, r32, 0.0)]
    return first, second


def kernel(sizes, bond, fresh, link, vert, narrow_h, wide_h, ket_h, mps_h, left_h, right_h, out_h, log_out,
           rows, bond_v, fresh_v, link_v, vert_v, bond_n, fresh_n, link_n, link_s, vert_s,
           narrow, wide, KH, KF, left_v, MB, RB, LF, L2F, L2, MS, RS, KM, KB2, KB3, W1, W2, W3, O4, IMG,
           SA, SB,
           lsem, csend, crecv, msend, mrecv, rsend, rrecv, fsend, frecv, asend, arecv, bsend, brecv):
    nx, nz, ny, _ = sizes
    x, z, y = lax.axis_index("col_0"), lax.axis_index("col_1"), lax.axis_index("col_2")
    sec = lax.axis_index("sec")
    other = 1 - sec
    count = nx * nz * ny
    site = (x * nz + z) * ny + y

    def place(j):
        return {"col_0": lax.div(j, nz * ny), "col_1": lax.rem(lax.div(j, ny), nz), "col_2": lax.rem(j, ny)}

    before = place(lax.rem(site + count - 1, count))
    after = place(lax.rem(site + 1, count))
    partner = {"sec": other}
    plane = x * ny + y

    def plane_peer(dx, dy, flip):
        return {"col_0": lax.rem(x + dx, nx), "col_2": lax.rem(y + dy, ny), "sec": other if flip else sec}

    offsets = [(dx, dy, f) for dx in range(nx) for dy in range(ny) for f in range(2) if dx + dy + f > 0]
    offsets.sort(key=lambda o: -min(o[0], nx - o[0]) - min(o[1], ny - o[1]))
    offsets.remove((0, 0, 1))
    offsets = [(0, 0, 1)] + offsets
    line_offsets = sorted(range(1, nz), key=lambda k: -min(k, nz - k))

    def line_peer(k):
        return {"col_1": lax.rem(z + k, nz)}

    barrier = pltpu.get_barrier_semaphore()
    peers = [line_peer(k) for k in line_offsets] + [plane_peer(*o) for o in offsets] + [before, after]
    for peer in peers:
        pl.semaphore_signal(barrier, inc=1, device_id=peer, device_id_type=MESH)

    fetched = [pltpu.make_async_copy(src, dst, lsem.at[i]) for i, (src, dst) in enumerate([
        (link, link_s), (bond, bond_v), (fresh, fresh_v), (left_h, left_v), (link, link_v), (mps_h, MB.at[sec]),
        (vert, vert_s), (vert, vert_v), (ket_h, KH), (narrow_h, narrow), (wide_h, wide)])]
    for c in fetched:
        c.start()

    rows[...] = jnp.zeros_like(rows)
    LF[...] = jnp.zeros_like(LF)
    L2F[...] = jnp.zeros_like(L2F)
    MS[:, :, 96:128, :] = jnp.zeros((3, 3, 32, 512), BF16)
    MS[:, :, 224:256, :] = jnp.zeros((3, 3, 32, 512), BF16)
    KF[...] = jnp.zeros_like(KF)
    KM[...] = jnp.zeros_like(KM)

    for c in fetched[:4]:
        c.wait()
    rows[0:1, 0:96] = bond_v[...]
    rows[1:2, 0:96] = fresh_v[...]
    qb = rows[0:1, :]
    col_qb = column(qb)
    col_fresh = column(rows[1:2, :])
    fresh_half = jnp.where(sec == 0, col_fresh[0:48, :], col_fresh[48:96, :])
    left_diff = fresh_half[:, :96] - qb[:, :96]
    for l in range(6):
        for m in range(6):
            keep = left_diff == link_s[0, l] - link_s[0, m]
            LF[pl.ds((l * 6 + m) * 48, 48), 0:96] = jnp.where(keep, left_v[l, m].astype(F32), 0.0)

    for c in fetched[4:6]:
        c.wait()
    pl.semaphore_wait(barrier, len(peers))

    def remote(src, dst, send, recv, peer):
        return pltpu.make_async_remote_copy(src_ref=src, dst_ref=dst, send_sem=send, recv_sem=recv,
                                            device_id=peer, device_id_type=MESH)

    charges = [remote(bond_v, bond_n, csend.at[0], crecv.at[0], before),
               remote(link_v, link_n, csend.at[1], crecv.at[1], before),
               remote(fresh_v, fresh_n, csend.at[2], crecv.at[2], before)]
    for c in charges:
        c.start()
    mps_send = remote(MB.at[sec], MB.at[sec], msend, mrecv, partner)
    mps_send.start()
    right_send = remote(right_h, RB.at[sec], rsend, rrecv, before)
    right_send.start()
    right_forward = remote(RB.at[sec], RB.at[sec], fsend, frecv, partner)

    for i in range(48):
        L2F[i % 4, pl.ds(40 * (i // 4), 36), :] = LF[pl.ds(i, 36, stride=48), :]
    L2[...] = L2F[...].astype(BF16)
    W1[:, :, 240:256, :] = jnp.zeros((6, 6, 16, 768), BF16)
    for c in fetched[6:]:
        c.wait()
    KF[:, 0:6] = KH[...].astype(F32)
    ket = None
    for i in range(12):
        part = KF[pl.ds(i, 36, stride=12), :]
        part = part if i == 0 else pltpu.roll(part, 8 * i, axis=1)
        ket = part if ket is None else ket + part

    for c in charges:
        c.wait_recv()
    rows[2:3, 0:96] = bond_n[...]
    rows[3:4, 0:96] = fresh_n[...]
    rows[4:5, 0:6] = link_v[...]
    rows[5:6, 0:6] = link_n[...]
    rows[6:8, 0:6] = vert_v[0]
    qbn = rows[2:3, :]

    def operators():
        charge_rows = rows[...].astype(F32)
        ket_rows = jnp.sum(narrow[848:896, :].astype(F32) * charge_rows[6:7, :]
                           + narrow[896:944, :].astype(F32) * charge_rows[4:5, :], axis=1, keepdims=True)
        lower = jnp.broadcast_to(charge_rows[7:8, :], (16, 128)).astype(BF16)
        ahead = jnp.broadcast_to(charge_rows[5:6, :], (16, 128)).astype(BF16)
        ket_cols = (jnp.dot(lower, narrow[592:720, :], preferred_element_type=F32)
                    + jnp.dot(ahead, narrow[720:848, :], preferred_element_type=F32)
                    + narrow[944:960, :].astype(F32))[0:1, :]
        keep = jnp.abs(ket_rows[0:36] - ket_cols) < 0.5
        KM[0:36, :] = jnp.where(keep, ket, 0.0).astype(BF16)
        spread = lax.dot_general(narrow[0:432, :], KM[...], (((1,), (1,)), ((), ())), preferred_element_type=F32)
        KB2[...] = (jnp.dot(spread.astype(BF16), wide[0:48, :], preferred_element_type=F32)
                    * wide[48:480, :].astype(F32)).astype(BF16)
        total = None
        for p in range(2):
            spread = lax.dot_general(narrow[432 + 80 * p:512 + 80 * p, :], KM[...], (((1,), (1,)), ((), ())),
                                     preferred_element_type=F32)
            part = jnp.dot(spread.astype(BF16), wide[480 + 48 * p:528 + 48 * p, :], preferred_element_type=F32)
            total = part if total is None else total + part
        KB3[...] = (total * wide[576:656, :].astype(F32)).astype(BF16)

    bond_diff = qbn[:, :96] - col_qb[:96, :96]
    mps_send.wait_recv()

    def boundary(i):
        up, vp = i // 3, i % 3
        for v in (2 * vp, 2 * vp + 1):
            for u in (2 * up, 2 * up + 1):
                keep = bond_diff == vert_s[0, 0, u] - vert_s[0, 0, v]
                t = jnp.concatenate([MB[0, u, v], MB[1, u, v]], axis=0).astype(F32)
                first, second = lane_parts(jnp.where(keep, t, 0.0))
                at = ((u % 2) + 2 * (v % 2)) * 128
                for k in range(3):
                    MS[i % 3, k, 0:96, at:at + 128] = first[k].astype(BF16)
                    MS[i % 3, k, 128:224, at:at + 128] = second[k].astype(BF16)

    def step1(i):
        up, vp = i // 3, i % 3
        for t in range(3):
            rhs = MS[i % 3, t]
            for c in range(480 // CHUNK1):
                lo = CHUNK1 * c
                lhs = jnp.concatenate([L2[t, lo:lo + CHUNK1, :], L2[t + 1, lo:lo + CHUNK1, :]], axis=1)
                o = jnp.dot(lhs, rhs, preferred_element_type=F32)
                for k in range(CHUNK1 // 40):
                    q = (CHUNK1 // 40) * c + k
                    for h in range(2):
                        w = jnp.concatenate([o[40 * k:40 * k + 40, 256 * h:256 * h + 128],
                                             o[40 * k:40 * k + 40, 256 * h + 128:256 * h + 256]], axis=0)
                        at = (q % 2) * 384 + t * 128
                        W1[q // 2, 2 * vp + h, up * 80:up * 80 + 80, at:at + 128] = w.astype(BF16)

    boundary(0)
    operators()
    for i in range(9):
        if i < 8:
            boundary(i + 1)
        step1(i)

    def do2(qp):
        for vp in range(3):
            oa = jnp.dot(KB2[...], W1[qp, 2 * vp], preferred_element_type=F32)
            ob = jnp.dot(KB2[...], W1[qp, 2 * vp + 1], preferred_element_type=F32)
            for g in range(18):
                t = jnp.concatenate([oa[24 * g:24 * g + 24], ob[24 * g:24 * g + 24]], axis=0)
                W2[qp % 2, g, 48 * vp:48 * vp + 48, :] = t.astype(BF16)

    def do3(qp):
        for g in range(18):
            r, dp = g // 3, g % 3
            o = jnp.dot(KB3[0:72, 0:144], W2[qp % 2, g], preferred_element_type=F32)
            row = qp * 72 + dp * 24
            for i in range(6):
                at = (r * 6 + i) * 128
                for t in range(3):
                    w = jnp.concatenate([o[12 * i:12 * i + 12, 128 * t:128 * t + 128],
                                         o[12 * i:12 * i + 12, 384 + 128 * t:512 + 128 * t]], axis=0)
                    W3[t, row:row + 24, at:at + 128] = w.astype(BF16)

    def right(r_range):
        right_diff = column(rows[3:4, :])[:96, :96] - qbn[:, :96]
        ahead_row = rows[5:6, :]
        for r in r_range:
            for s in range(6):
                keep = right_diff == ahead_row[:, r:r + 1] - ahead_row[:, s:s + 1]
                t = jnp.concatenate([RB[0, r, s], RB[1, r, s]], axis=0).astype(F32)
                first, second = lane_parts(jnp.where(keep, t, 0.0))
                at = (r * 6 + s) * 128
                for k in range(3):
                    RS[k, 0:96, at:at + 128] = first[k].astype(BF16)
                    RS[k, 128:224, at:at + 128] = second[k].astype(BF16)

    do2(0)
    for qp in range(1, 6):
        if qp == FORWARD_AT:
            right_send.wait_recv()
            right_forward.start()
        do2(qp)
        do3(qp - 1)
    right_forward.wait_recv()
    right(range(6))
    do3(5)

    for t in range(3):
        O4[t] = lax.dot_general(W3[t], RS[t], (((1,), (1,)), ((), ())), preferred_element_type=F32)
    acc = jnp.zeros((12, 96), F32)
    for qp in range(6):
        for dp in range(3):
            for h in range(2):
                row = qp * 72 + dp * 24 + h * 12
                o = [O4[t, row:row + 12, :] for t in range(3)]
                parts = [o[0][:, 0:96], o[0][:, 128:224] + o[1][:, 0:96],
                         o[1][:, 128:224] + o[2][:, 0:96], o[2][:, 128:224]]
                for k in range(4):
                    at = (8 * qp + 4 * h + k) * 36 + dp * 12
                    IMG[at:at + 12, 0:96] = parts[k]
                    acc = acc + parts[k] * parts[k]
    mine = jnp.sum(jnp.sum(acc, axis=0, keepdims=True), axis=1, keepdims=True)
    own = SA.at[sec, pl.ds(plane, 1), :]
    own[...] = jnp.broadcast_to(mine, (1, 128))
    plane_sends = []
    for dx, dy, f in offsets:
        i = 2 * (dx * ny + dy) + f
        plane_sends.append(remote(own, own, asend.at[i], arecv.at[i], plane_peer(dx, dy, f)))
    for c in plane_sends:
        c.start()
    plane_sends[0].wait_recv()

    meansq = (SA[0, pl.ds(plane, 1), :] + SA[1, pl.ds(plane, 1), :]) / 331776.0
    scale = lax.rsqrt(meansq + 1e-06)
    for d in range(6):
        for e in range(6):
            t = IMG[pl.ds(d * 6 + e, 48, stride=36), 0:96]
            out_h[d, e] = (t * scale[:, 0:96]).astype(BF16)

    for c in plane_sends[1:]:
        c.wait_recv()
    logs = 0.5 * jnp.log((SA[0] + SA[1]) / 331776.0 + 1e-06)
    SB[pl.ds(z, 1), :] = jnp.sum(logs, axis=0, keepdims=True)
    line = SB.at[pl.ds(z, 1), :]
    line_sends = [remote(line, line, bsend.at[k], brecv.at[k], line_peer(k)) for k in line_offsets]
    for c in line_sends:
        c.start()
    for c in line_sends:
        c.wait_recv()
    log_out[...] = jnp.sum(SB[...], axis=0, keepdims=True) / float(count)

    for c in charges + [mps_send, right_send, right_forward] + plane_sends + line_sends:
        c.wait_send()


def local(sizes, mps, ket, left_proj, right_proj, bond_charge, new_charge, link_charge, vert_charge):
    nx, nz, ny, _ = sizes
    mps_v = mps[0].transpose(1, 2, 0, 3)
    left_v = left_proj[0].transpose(2, 3, 0, 1)
    right_v = right_proj[0].transpose(1, 2, 3, 0)
    ket_v = ket.transpose(0, 1, 2, 3, 5, 4).reshape(432, 6)
    vm = pl.BlockSpec(memory_space=pltpu.VMEM)
    hbm = pl.BlockSpec(memory_space=pl.ANY)
    dma = pltpu.SemaphoreType.DMA
    out, log_row = pl.pallas_call(
        lambda *refs: kernel(sizes, *refs),
        out_shape=(pltpu.VMEM((6, 6, 48, 96), BF16), pltpu.VMEM((1, 128), F32)),
        in_specs=[hbm] * 10,
        out_specs=(vm, vm),
        scratch_shapes=[
            pltpu.VMEM((8, 128), I32),
            pltpu.VMEM((1, 96), I32), pltpu.VMEM((1, 96), I32), pltpu.VMEM((1, 6), I32), pltpu.VMEM((1, 2, 6), I32),
            pltpu.VMEM((1, 96), I32), pltpu.VMEM((1, 96), I32), pltpu.VMEM((1, 6), I32),
            pltpu.SMEM((1, 6), I32), pltpu.SMEM((1, 2, 6), I32),
            pltpu.VMEM((960, 128), BF16), pltpu.VMEM((656, 256), BF16),
            pltpu.VMEM((432, 6), BF16), pltpu.VMEM((432, 128), F32),
            pltpu.VMEM((6, 6, 48, 96), BF16),
            pltpu.VMEM((2, 6, 6, 48, 96), BF16), pltpu.VMEM((2, 6, 6, 48, 96), BF16),
            pltpu.VMEM((1728, 128), F32), pltpu.VMEM((4, 480, 128), F32), pltpu.VMEM((4, 480, 128), BF16),
            pltpu.VMEM((3, 3, 256, 512), BF16), pltpu.VMEM((3, 256, 4608), BF16),
            pltpu.VMEM((48, 128), BF16), pltpu.VMEM((432, 256), BF16), pltpu.VMEM((80, 256), BF16),
            pltpu.VMEM((6, 6, 256, 768), BF16), pltpu.VMEM((2, 18, 144, 768), BF16),
            pltpu.VMEM((3, 432, 4608), BF16), pltpu.VMEM((3, 432, 256), F32), pltpu.VMEM((1728, 128), F32),
            pltpu.VMEM((2, nx * ny, 128), F32), pltpu.VMEM((nz, 128), F32),
            dma((11,)), dma((3,)), dma((3,)), dma(()), dma(()), dma(()), dma(()), dma(()), dma(()),
            dma((2 * nx * ny,)), dma((2 * nx * ny,)), dma((nz,)), dma((nz,))],
        compiler_params=pltpu.CompilerParams(
            vmem_limit_bytes=VMEM_LIMIT, collective_id=0, has_side_effects=True),
    )(bond_charge, new_charge, link_charge, vert_charge, *operator_tables(), ket_v, mps_v, left_v, right_v)
    return out.transpose(2, 0, 1, 3)[None], log_row[0, 0]


def solution(mesh):
    if mesh.shape["col"] == 128:
        sizes = (4, 8, 4, mesh.shape["sec"])
    else:
        sizes = (2, mesh.shape["col"] // 4, 2, mesh.shape["sec"])
    torus = Mesh(mesh.devices.reshape(sizes), (*COL, "sec"))
    in_specs = (
        P(COL, "sec", None, None, None),
        P(COL, None, None, None, None, None),
        P(COL, "sec", None, None, None),
        P(COL, None, None, None, "sec"),
        P(COL, None),
        P(COL, None),
        P(COL, None),
        P(COL, None, None),
    )
    out_specs = (P(COL, "sec", None, None, None), P())
    return jax.shard_map(lambda *a: local(sizes, *a), mesh=torus, in_specs=in_specs, out_specs=out_specs,
                         check_vma=False)
```
